8 devices in a mesh: tp: 4 (over z, y, x), dp: 2 (over core).
Axes of the slice: x: 2, y: 2, z: 1, core: 2. Of those that a mesh axis runs over, the one named last changes fastest.
Arguments:
- x: bfloat16 [16384, 5120], P(('dp', 'tp'))
- w_gate: bfloat16 [5120, 13824], P('dp', 'tp')
- w_up: bfloat16 [5120, 13824], P('dp', 'tp')
- w_down: bfloat16 [13824, 5120], P('tp', 'dp')
Outputs:
- output: bfloat16 [16384, 5120], P(('dp', 'tp'))
All inputs are finite; a program needn't handle non-finite values.
Results may differ from the reference program's by a relative error of at most 0.0131407.
Values are sent between devices in bfloat16 or wider.
A program may use at most 1 GiB of HBM per device.

```python
import jax
import jax.numpy as jnp
from jax import lax

D = 5120
FF = 13824
TOKENS_DEV = 2048
ROWS = 16384

NBLK = ROWS // TOKENS_DEV


def setup_inputs(seed: int = 0) -> dict:
    k = jax.random.split(jax.random.key(seed), 4)
    x = jax.random.normal(k[0], (ROWS, D), jnp.float32)
    wg = jax.random.normal(k[1], (D, FF), jnp.float32) * D ** -0.5
    wu = jax.random.normal(k[2], (D, FF), jnp.float32) * D ** -0.5
    wd = jax.random.normal(k[3], (FF, D), jnp.float32) * FF ** -0.5
    return {"x": x.astype(jnp.bfloat16), "w_gate": wg.astype(jnp.bfloat16), "w_up": wu.astype(jnp.bfloat16), "w_down": wd.astype(jnp.bfloat16)}


def reference(x, w_gate, w_up, w_down):
    def blk(xb):
        a = jnp.dot(xb, w_gate, preferred_element_type=jnp.float32)
        b = jnp.dot(xb, w_up, preferred_element_type=jnp.float32)
        h = (jax.nn.silu(a) * b).astype(jnp.bfloat16)
        o = jnp.dot(h, w_down, preferred_element_type=jnp.float32)
        return (xb.astype(jnp.float32) + o).astype(jnp.bfloat16)
    y = lax.map(blk, x.reshape(NBLK, TOKENS_DEV, D))
    return y.reshape(ROWS, D)
```

```python
import jax
import jax.numpy as jnp
from jax import lax
from jax.experimental import pallas as pl
from jax.experimental.pallas import tpu as pltpu
from jax.sharding import PartitionSpec as P

MESH = pl.DeviceIdType.MESH
M = 1024
C = 256
FT = 256
WC = 512
S = 128
NC = 1280

BLOCKS = (
    ("bx0", "bx1", "ay0", "ay1"),
    ("ad0", "ad1", "bd0", "bd1"),
    ("bx2", "bx3", "ay2", "ay3"),
    ("ad2", "ad3", "bd2", "bd3"),
    ("ax0", "ax1", "by0", "by1"),
    ("ax2", "ax3", "by2", "by3"),
)
PLACE = {name: (b, q) for b, names in enumerate(BLOCKS) for q, name in enumerate(names)}

GATHER = {
    -1: (("ax0", "bx0", "ax1"), ("by0", "ay0", "by1")),
    7: (("bd0",), ("ad0",)),
    13: (("bx1",), ("ay1",)),
    20: (("ax2",), ("by2",)),
    27: (("bd1",), ("ad1",)),
    28: (("bx2",), ("ay2",)),
    34: (("ax3",), ("by3",)),
    41: (("bx3",), ("ay3",)),
    48: (("bd2",), ("ad2",)),
    55: (("bd3",), ("ad3",)),
}
REDUCE = {
    3: (("bd0", "bd1", "bx0", "bx1"), ("ad0", "ad1", "ay0", "ay1")),
    5: (("bd2", "bd3", "bx2", "bx3"), ("ad2", "ad3", "ay2", "ay3")),
    6: (("ax0", "ax1"), ("by0", "by1")),
    7: (("ax2", "ax3"), ("by2", "by3")),
}


def kernel(x, wg, wu, wd, out, gath, prod, part, near, far, pg, pu, pd,
           xv, acc, gv, uv, dv, hv, ov, rv,
           g_send, g_recv, r_send, r_recv, w_send, w_recv, w_load, x_load, o_sem, r_load, f_sem):
    tp, dp = lax.axis_index("tp"), lax.axis_index("dp")
    nx = tp + 1 - 2 * (tp % 2)
    ny = tp + 2 - 4 * (tp // 2)
    half = x.shape[0] // 2
    kd, ff = wg.shape
    dc = wd.shape[1]
    nf = pl.cdiv(ff, FT)
    to_x, to_y, to_core = {"tp": nx}, {"tp": ny}, {"dp": 1 - dp}

    barrier = pltpu.get_barrier_semaphore()
    for who in (to_x, to_y, to_core):
        pl.semaphore_signal(barrier, inc=1, device_id=who, device_id_type=MESH)
    pl.semaphore_wait(barrier, 3)

    def link_of(name):
        return to_x if name[:2] in ("ax", "bx", "bd") else to_y

    def gather(name):
        who = link_of(name)
        b, q = PLACE[name]
        n = int(name[2])
        if name[1] == "d":
            fb, fq = PLACE[("b" if name[0] == "b" else "a") + ("y" if name[0] == "b" else "x") + name[2]]
            src = gath.at[fb, pl.ds(fq * C, C)]
        else:
            src = x.at[pl.ds((half if name[0] == "b" else 0) + n * C, C)]
        return pltpu.make_async_remote_copy(
            src_ref=src, dst_ref=gath.at[b, pl.ds(q * C, C)],
            send_sem=g_send.at[b, q], recv_sem=g_recv.at[b, q], device_id=who, device_id_type=MESH)

    def send_gather(step):
        xs, ys = GATHER[step]
        for name in (v for pair in zip(xs, ys) for v in pair):
            if name[1] == "d":
                gather(("by" if name[0] == "b" else "ax") + name[2]).wait_recv()
        for name in (v for pair in zip(xs, ys) for v in pair):
            gather(name).start()

    def reduce(name):
        b, q = PLACE[name]
        n = int(name[2])
        own = (4 if name[0] == "b" else 0) + n
        if name[1] == "d":
            dst = part.at[n // 2, pl.ds(((2 if name[0] == "b" else 0) + n % 2) * C, C)]
        elif name[:2] in ("ay", "bx"):
            dst = near.at[own]
        else:
            dst = far.at[own]
        who = link_of(name)
        return pltpu.make_async_remote_copy(
            src_ref=prod.at[b + 2, pl.ds(q * C, C)], dst_ref=dst,
            send_sem=r_send.at[b, q], recv_sem=r_recv.at[b, q], device_id=who, device_id_type=MESH)

    def weights(k, j):
        width = min(WC, ff - j * WC)
        span = pl.ds(j * WC, width)
        ref, peer = ((wg, pg), (wu, pu), (wd, pd))[k]
        at = (span,) if k == 2 else (slice(None), span)
        return pltpu.make_async_remote_copy(
            src_ref=ref.at[at], dst_ref=peer.at[at], send_sem=w_send.at[k, j], recv_sem=w_recv.at[k, j],
            device_id=to_core, device_id_type=MESH)

    nw = pl.cdiv(ff, WC)
    send_gather(-1)
    for j in range(nw):
        for k in range(3):
            weights(k, j).start()

    def load_weights(f, slot):
        at = pl.multiple_of(lax.min(f * FT, ff - FT), 128)
        copies = []
        for k, (ref, peer, dst) in enumerate(((wg, pg, gv), (wu, pu, uv))):
            for m, (src, core) in enumerate(((ref, dp), (peer, 1 - dp))):
                rows = pl.ds(pl.multiple_of(core * kd, 128), kd)
                copies.append(pltpu.make_async_copy(
                    src.at[:, pl.ds(at, FT)], dst.at[slot, rows], w_load.at[slot, 2 * k + m]))
        for m, (src, core) in enumerate(((wd, dp), (pd, 1 - dp))):
            cols = pl.ds(pl.multiple_of(core * dc, 128), dc)
            copies.append(pltpu.make_async_copy(
                src.at[pl.ds(at, FT)], dv.at[slot, :, cols], w_load.at[slot, 4 + m]))
        return copies

    def await_weights(j):
        for k in range(3):
            weights(k, j).wait_recv()

    def load_own(i, q):
        at = pl.multiple_of(lax.min(i, 1) * M + q * C, C)
        return pltpu.make_async_copy(x.at[pl.ds(at, C)], xv.at[pl.ds(q * C, C)], x_load.at[q])

    def load_rows(b, q):
        rows = pl.ds(q * C, C)
        return pltpu.make_async_copy(gath.at[b, rows], xv.at[rows], x_load.at[q])

    def start_rows(i):
        @pl.when(i < 2)
        def _():
            for q in range(M // C):
                load_own(i, q).start()
        for b in range(len(BLOCKS)):
            @pl.when(i == b + 2)
            def _():
                for q, name in enumerate(BLOCKS[b]):
                    if name[:2] not in ("ax", "by"):
                        gather(name).wait_recv()
                    load_rows(b, q).start()

    start_rows(jnp.int32(0))
    await_weights(0)
    for copy in load_weights(jnp.int32(0), 0):
        copy.start()

    def store(i, r, slot):
        return pltpu.make_async_copy(ov.at[slot], prod.at[i, pl.ds(pl.multiple_of(r * S, S), S)], o_sem.at[slot])

    def load_part(i, r, slot):
        return pltpu.make_async_copy(part.at[lax.max(i - 6, 0), pl.ds(pl.multiple_of(r * S, S), S)], rv.at[slot], r_load.at[slot])

    @pl.loop(0, len(BLOCKS) + 2)
    def _(i):
        acc[...] = jnp.zeros_like(acc)
        for q in range(M // C):
            load_own(i, q).wait()

        @pl.loop(0, nf)
        def _(f):
            step = i * nf + f
            slot = step % 2
            for at in GATHER:
                if at >= 0:
                    @pl.when(step == at)
                    def _():
                        send_gather(at)
            for j in range(1, nw):
                @pl.when(step == j * WC // FT - 1)
                def _():
                    await_weights(j)
            for copy in load_weights(f, slot):
                copy.wait()

            @pl.when(step + 1 < (len(BLOCKS) + 2) * nf)
            def _():
                for copy in load_weights((f + 1) % nf, 1 - slot):
                    copy.start()
            a = jnp.dot(xv[...], gv[slot], preferred_element_type=jnp.float32)
            b = jnp.dot(xv[...], uv[slot], preferred_element_type=jnp.float32)
            skip = lax.max(f * FT - (ff - FT), 0)
            fresh = lax.broadcasted_iota(jnp.int32, (M, FT), 1) >= skip
            h = a * jax.nn.sigmoid(a) * b
            hv[...] = jnp.where(fresh, h, 0.0).astype(jnp.bfloat16)
            for n in range(0, acc.shape[1], NC):
                cols = slice(n, n + NC)
                acc[:, cols] += jnp.dot(hv[...], dv[slot, :, cols], preferred_element_type=jnp.float32)

        late = i >= 6
        for k in range(2):
            @pl.when(i == 6 + k)
            def _():
                for q in range(2):
                    reduce("ad" + str(2 * k + q)).wait_recv()
                    reduce("bd" + str(2 * k + q)).wait_recv()
        @pl.when(late)
        def _():
            load_part(i, 0, 0).start()

        @pl.loop(0, M // S)
        def _(r):
            slot = r % 2
            rows = pl.ds(pl.multiple_of(r * S, S), S)

            @pl.when(r >= 2)
            def _():
                store(i, r - 2, slot).wait()

            @pl.when(late)
            def _():
                @pl.when(r + 1 < M // S)
                def _():
                    load_part(i, r + 1, 1 - slot).start()
                load_part(i, r, slot).wait()
                ov[slot] = (acc[rows] + rv[slot].astype(jnp.float32)).astype(jnp.bfloat16)

            @pl.when(jnp.logical_not(late))
            def _():
                ov[slot] = acc[rows].astype(jnp.bfloat16)
            store(i, r, slot).start()
        for slot in range(2):
            store(i, M // S - 2 + slot, slot).wait()

        for at in REDUCE:
            @pl.when(i == at)
            def _():
                for pair in zip(*REDUCE[at]):
                    for name in pair:
                        reduce(name).start()

        @pl.when(i + 1 < len(BLOCKS) + 2)
        def _():
            start_rows(i + 1)

    order = [half_ + str(n) for n in range(4) for half_ in "ab"]

    def parts(name):
        own = (4 if name[0] == "b" else 0) + int(name[1])
        srcs = (prod.at[own // 4, pl.ds((own % 4) * C, C)], near.at[own], far.at[own])
        return [pltpu.make_async_copy(src, xv.at[pl.ds(m * C, C)], f_sem.at[m]) for m, src in enumerate(srcs)]

    def result(name):
        n = int(name[1])
        return pltpu.make_async_copy(
            xv.at[pl.ds(3 * C, C)], out.at[pl.ds((half if name[0] == "b" else 0) + n * C, C)], f_sem.at[3])

    for t, name in enumerate(order):
        n = name[1]
        reduce(("ay" if name[0] == "a" else "bx") + n).wait_recv()
        reduce(("ax" if name[0] == "a" else "by") + n).wait_recv()
        copies = parts(name)
        for copy in copies:
            copy.start()
        for copy in copies:
            copy.wait()
        if t:
            result(order[t - 1]).wait()

        @pl.loop(0, C // 32)
        def _(r):
            rows = [pl.ds(pl.multiple_of(m * C + r * 32, 32), 32) for m in range(4)]
            f32 = jnp.float32
            xv[rows[3]] = (xv[rows[0]].astype(f32) + xv[rows[1]].astype(f32) + xv[rows[2]].astype(f32)).astype(jnp.bfloat16)
        result(name).start()
    result(order[-1]).wait()

    for name in PLACE:
        gather(name).wait_send()
        reduce(name).wait_send()
    for j in range(nw):
        for k in range(3):
            weights(k, j).wait_send()


def solution(mesh):
    def body(x, wg, wu, wd):
        r, d = x.shape
        kd, ff = wg.shape
        dc = wd.shape[1]
        bf = jnp.bfloat16
        any_ = pl.BlockSpec(memory_space=pl.ANY)
        nb = len(BLOCKS)
        nw = -(-ff // WC)
        shapes = [(r, d), (nb, M, d), (nb + 2, M, d), (2, M, d), (r // C, C, d), (r // C, C, d), (kd, ff), (kd, ff), (ff, dc)]
        dma = pltpu.SemaphoreType.DMA
        outs = pl.pallas_call(
            kernel,
            out_shape=[jax.ShapeDtypeStruct(s, bf) for s in shapes],
            in_specs=[any_] * 4,
            out_specs=[any_] * len(shapes),
            scratch_shapes=[
                pltpu.VMEM((M, d), bf), pltpu.VMEM((M, d), jnp.float32),
                pltpu.VMEM((2, d, FT), bf), pltpu.VMEM((2, d, FT), bf), pltpu.VMEM((2, FT, d), bf),
                pltpu.VMEM((M, FT), bf), pltpu.VMEM((2, S, d), bf), pltpu.VMEM((2, S, d), bf),
                dma((nb, M // C)), dma((nb, M // C)), dma((nb, M // C)), dma((nb, M // C)),
                dma((3, nw)), dma((3, nw)), dma((2, 6)), dma((M // C,)), dma((2,)), dma((2,)), dma((4,)),
            ],
            compiler_params=pltpu.CompilerParams(collective_id=0, has_side_effects=True, vmem_limit_bytes=67043328),
        )(x, wg, wu, wd)
        return (x.astype(jnp.float32) + outs[0].astype(jnp.float32)).astype(bf)

    return jax.shard_map(body, mesh=mesh, in_specs=(P(("dp", "tp"), None), P("dp", "tp"), P("dp", "tp"), P("tp", "dp")), out_specs=P(("dp", "tp"), None), check_vma=False)
```

```python
import jax
import jax.numpy as jnp
from jax import lax
from jax.experimental import pallas as pl
from jax.experimental.pallas import tpu as pltpu
from jax.sharding import PartitionSpec as P

MESH = pl.DeviceIdType.MESH
M = 1024
C = 256
FT = 256
WC = 512
S = 128
NC = 1280
R = 32

BLOCKS = (
    ("bx0", "bx1", "ay0", "ay1"),
    ("ad0", "ad1", "bd0", "bd1"),
    ("bx2", "bx3", "ay2", "ay3"),
    ("ad2", "ad3", "bd2", "bd3"),
    ("ax0", "ax1", "by0", "by1"),
    ("ax2", "ax3", "by2", "by3"),
)
PLACE = {name: (b, q) for b, names in enumerate(BLOCKS) for q, name in enumerate(names)}

GATHER = {
    -1: (("ax0", "bx0", "ax1"), ("by0", "ay0", "by1")),
    7: (("bd0",), ("ad0",)),
    13: (("bx1",), ("ay1",)),
    20: (("ax2",), ("by2",)),
    27: (("bd1",), ("ad1",)),
    28: (("bx2",), ("ay2",)),
    34: (("ax3",), ("by3",)),
    41: (("bx3",), ("ay3",)),
    48: (("bd2",), ("ad2",)),
    55: (("bd3",), ("ad3",)),
}
REDUCE = {
    3: (("bd0", "bd1", "bx0", "bx1"), ("ad0", "ad1", "ay0", "ay1")),
    5: (("bd2", "bd3", "bx2", "bx3"), ("ad2", "ad3", "ay2", "ay3")),
    6: (("ax0", "ax1"), ("by0", "by1")),
    7: (("ax2", "ax3"), ("by2", "by3")),
}


def kernel(x, wg, wu, wd, xv, acc, gath, prod, part, near, far, pg, pu, pd,
           gv, uv, dv, hv, ov, rv,
           g_send, g_recv, r_send, r_recv, w_send, w_recv, w_load, x_load, o_sem, r_load, f_sem):
    tp, dp = lax.axis_index("tp"), lax.axis_index("dp")
    nx = tp + 1 - 2 * (tp % 2)
    ny = tp + 2 - 4 * (tp // 2)
    half = x.shape[0] // 2
    kd, ff = wg.shape
    dc = wd.shape[1]
    nf = pl.cdiv(ff, FT)
    to_x, to_y, to_core = {"tp": nx}, {"tp": ny}, {"dp": 1 - dp}

    barrier = pltpu.get_barrier_semaphore()
    for who in (to_x, to_y, to_core):
        pl.semaphore_signal(barrier, inc=1, device_id=who, device_id_type=MESH)
    pl.semaphore_wait(barrier, 3)

    def link_of(name):
        return to_x if name[:2] in ("ax", "bx", "bd") else to_y

    def gather(name):
        who = link_of(name)
        b, q = PLACE[name]
        n = int(name[2])
        if name[1] == "d":
            fb, fq = PLACE[("b" if name[0] == "b" else "a") + ("y" if name[0] == "b" else "x") + name[2]]
            src = gath.at[fb, pl.ds(fq * C, C)]
        else:
            src = x.at[pl.ds((half if name[0] == "b" else 0) + n * C, C)]
        return pltpu.make_async_remote_copy(
            src_ref=src, dst_ref=gath.at[b, pl.ds(q * C, C)],
            send_sem=g_send.at[b, q], recv_sem=g_recv.at[b, q], device_id=who, device_id_type=MESH)

    def send_gather(step):
        xs, ys = GATHER[step]
        for name in (v for pair in zip(xs, ys) for v in pair):
            if name[1] == "d":
                gather(("by" if name[0] == "b" else "ax") + name[2]).wait_recv()
        for name in (v for pair in zip(xs, ys) for v in pair):
            gather(name).start()

    def reduce(name):
        b, q = PLACE[name]
        n = int(name[2])
        own = (4 if name[0] == "b" else 0) + n
        if name[1] == "d":
            dst = part.at[n // 2, pl.ds(((2 if name[0] == "b" else 0) + n % 2) * C, C)]
        elif name[:2] in ("ay", "bx"):
            dst = near.at[own]
        else:
            dst = far.at[own]
        who = link_of(name)
        return pltpu.make_async_remote_copy(
            src_ref=prod.at[b + 2, pl.ds(q * C, C)], dst_ref=dst,
            send_sem=r_send.at[b, q], recv_sem=r_recv.at[b, q], device_id=who, device_id_type=MESH)

    def weights(k, j):
        width = min(WC, ff - j * WC)
        span = pl.ds(j * WC, width)
        ref, peer = ((wg, pg), (wu, pu), (wd, pd))[k]
        at = (span,) if k == 2 else (slice(None), span)
        return pltpu.make_async_remote_copy(
            src_ref=ref.at[at], dst_ref=peer.at[at], send_sem=w_send.at[k, j], recv_sem=w_recv.at[k, j],
            device_id=to_core, device_id_type=MESH)

    nw = pl.cdiv(ff, WC)
    send_gather(-1)
    for j in range(nw):
        for k in range(3):
            weights(k, j).start()

    def load_weights(f, slot):
        at = pl.multiple_of(lax.min(f * FT, ff - FT), 128)
        copies = []
        for k, (ref, peer, dst) in enumerate(((wg, pg, gv), (wu, pu, uv))):
            for m, (src, core) in enumerate(((ref, dp), (peer, 1 - dp))):
                rows = pl.ds(pl.multiple_of(core * kd, 128), kd)
                copies.append(pltpu.make_async_copy(
                    src.at[:, pl.ds(at, FT)], dst.at[slot, rows], w_load.at[slot, 2 * k + m]))
        for m, (src, core) in enumerate(((wd, dp), (pd, 1 - dp))):
            cols = pl.ds(pl.multiple_of(core * dc, 128), dc)
            copies.append(pltpu.make_async_copy(
                src.at[pl.ds(at, FT)], dv.at[slot, :, cols], w_load.at[slot, 4 + m]))
        return copies

    def await_weights(j):
        for k in range(3):
            weights(k, j).wait_recv()

    def load_own(i, q):
        at = pl.multiple_of(lax.min(i, 1) * M + q * C, C)
        return pltpu.make_async_copy(x.at[pl.ds(at, C)], xv.at[pl.ds(q * C, C)], x_load.at[q])

    def load_rows(b, q):
        rows = pl.ds(q * C, C)
        return pltpu.make_async_copy(gath.at[b, rows], xv.at[rows], x_load.at[q])

    def start_rows(i):
        @pl.when(i < 2)
        def _():
            for q in range(M // C):
                load_own(i, q).start()
        for b in range(len(BLOCKS)):
            @pl.when(i == b + 2)
            def _():
                for q, name in enumerate(BLOCKS[b]):
                    if name[:2] not in ("ax", "by"):
                        gather(name).wait_recv()
                    load_rows(b, q).start()

    start_rows(jnp.int32(0))
    await_weights(0)
    for copy in load_weights(jnp.int32(0), 0):
        copy.start()

    def store(i, r, slot):
        return pltpu.make_async_copy(ov.at[slot], prod.at[i, pl.ds(pl.multiple_of(r * S, S), S)], o_sem.at[slot])

    def load_part(i, r, slot):
        return pltpu.make_async_copy(part.at[lax.max(i - 6, 0), pl.ds(pl.multiple_of(r * S, S), S)], rv.at[slot], r_load.at[slot])

    @pl.loop(0, len(BLOCKS) + 2)
    def _(i):
        acc[...] = jnp.zeros_like(acc)
        for q in range(M // C):
            load_own(i, q).wait()

        @pl.loop(0, nf)
        def _(f):
            step = i * nf + f
            slot = step % 2
            for at in GATHER:
                if at >= 0:
                    @pl.when(step == at)
                    def _():
                        send_gather(at)
            for j in range(1, nw):
                @pl.when(step == j * WC // FT - 1)
                def _():
                    await_weights(j)
            for copy in load_weights(f, slot):
                copy.wait()

            @pl.when(step + 1 < (len(BLOCKS) + 2) * nf)
            def _():
                for copy in load_weights((f + 1) % nf, 1 - slot):
                    copy.start()
            a = jnp.dot(xv[...], gv[slot], preferred_element_type=jnp.float32)
            b = jnp.dot(xv[...], uv[slot], preferred_element_type=jnp.float32)
            skip = lax.max(f * FT - (ff - FT), 0)
            fresh = lax.broadcasted_iota(jnp.int32, (M, FT), 1) >= skip
            h = a * jax.nn.sigmoid(a) * b
            hv[...] = jnp.where(fresh, h, 0.0).astype(jnp.bfloat16)
            for n in range(0, acc.shape[1], NC):
                cols = slice(n, n + NC)
                acc[:, cols] += jnp.dot(hv[...], dv[slot, :, cols], preferred_element_type=jnp.float32)

        late = i >= 6
        for k in range(2):
            @pl.when(i == 6 + k)
            def _():
                for q in range(2):
                    reduce("ad" + str(2 * k + q)).wait_recv()
                    reduce("bd" + str(2 * k + q)).wait_recv()
        @pl.when(late)
        def _():
            load_part(i, 0, 0).start()

        @pl.loop(0, M // S)
        def _(r):
            slot = r % 2
            rows = pl.ds(pl.multiple_of(r * S, S), S)

            @pl.when(r >= 2)
            def _():
                store(i, r - 2, slot).wait()

            @pl.when(late)
            def _():
                @pl.when(r + 1 < M // S)
                def _():
                    load_part(i, r + 1, 1 - slot).start()
                load_part(i, r, slot).wait()
                ov[slot] = (acc[rows] + rv[slot].astype(jnp.float32)).astype(jnp.bfloat16)

            @pl.when(jnp.logical_not(late))
            def _():
                ov[slot] = acc[rows].astype(jnp.bfloat16)
            store(i, r, slot).start()
        for slot in range(2):
            store(i, M // S - 2 + slot, slot).wait()

        for at in REDUCE:
            @pl.when(i == at)
            def _():
                for pair in zip(*REDUCE[at]):
                    for name in pair:
                        reduce(name).start()

        @pl.when(i + 1 < len(BLOCKS) + 2)
        def _():
            start_rows(i + 1)

    f32 = jnp.float32

    def own_of(name):
        return (4 if name[0] == "b" else 0) + int(name[1])

    def pieces(name):
        own = own_of(name)
        src = pl.ds((half if name[0] == "b" else 0) + int(name[1]) * C, C)
        copies = [pltpu.make_async_copy(prod.at[own // 4, pl.ds((own % 4) * C, C)], dv.at[0], f_sem.at[0]),
                  pltpu.make_async_copy(near.at[own], dv.at[1], f_sem.at[1])]
        for m in range(2):
            part_ = pl.ds(src.start + m * S, S)
            copies.append(pltpu.make_async_copy(x.at[part_], ov.at[m], f_sem.at[2 + m]))
        return copies

    def late_piece(name, m, to):
        sem = f_sem.at[(4 if to is rv else 2) + m]
        return pltpu.make_async_copy(far.at[own_of(name), pl.ds(m * S, S)], to.at[m], sem)

    def await_near(name):
        reduce(("ay" if name[0] == "a" else "bx") + name[1]).wait_recv()

    def await_far(name):
        reduce(("ax" if name[0] == "a" else "by") + name[1]).wait_recv()

    def place(name):
        return (2 * C if name[0] == "b" else 0) + int(name[1]) % 2 * C

    def run(copies):
        for copy in copies:
            copy.start()
        for copy in copies:
            copy.wait()

    def rows_of(base, r):
        return pl.ds(pl.multiple_of(base + r * R, R), R)

    for name in ("a2", "b2", "a3", "b3"):
        await_near(name)
        run(pieces(name))
        for m in range(2):
            @pl.loop(0, S // R)
            def _(r):
                at, here = rows_of(m * S, r), rows_of(0, r)
                acc[rows_of(place(name) + m * S, r)] = (
                    dv[0, at].astype(f32) + dv[1, at].astype(f32) + ov[m, here].astype(f32))
    for name in ("a0", "b0", "a1", "b1"):
        await_near(name)
        await_far(name)
        run(pieces(name) + [late_piece(name, m, rv) for m in range(2)])
        for m in range(2):
            @pl.loop(0, S // R)
            def _(r):
                at, here = rows_of(m * S, r), rows_of(0, r)
                xv[rows_of(place(name) + m * S, r)] = (
                    dv[0, at].astype(f32) + dv[1, at].astype(f32) + rv[m, here].astype(f32) + ov[m, here].astype(f32)
                ).astype(jnp.bfloat16)
    for n in ("2", "3"):
        lates = []
        for name, to in (("a" + n, rv), ("b" + n, ov)):
            await_far(name)
            for m in range(2):
                lates.append((late_piece(name, m, to), to, place(name) + m * S, m))
                lates[-1][0].start()
        for copy, to, base, m in lates:
            copy.wait()

            @pl.loop(0, S // R)
            def _(r):
                at = rows_of(base, r)
                acc[at] = acc[at] + to[m, rows_of(0, r)].astype(f32)

    for name in PLACE:
        gather(name).wait_send()
        reduce(name).wait_send()
    for j in range(nw):
        for k in range(3):
            weights(k, j).wait_send()


def write(xv, acc, out, yv, sem):
    half, quarter = xv.shape[0], xv.shape[0] // 2
    early = [pltpu.make_async_copy(xv.at[pl.ds(k * quarter, quarter)], out.at[pl.ds(k * half, quarter)], sem.at[k]) for k in range(2)]
    late = []
    for k in range(8):
        rows = k * S
        to = (k // 4) * half + quarter + (k % 4) * S
        late.append(pltpu.make_async_copy(yv.at[pl.ds(rows, S)], out.at[pl.ds(to, S)], sem.at[2 + k]))
    for copy in early:
        copy.start()
    for k, copy in enumerate(late):
        @pl.loop(0, S // R)
        def _(r):
            at = pl.ds(pl.multiple_of(k * S + r * R, R), R)
            yv[at] = acc[at].astype(jnp.bfloat16)
        copy.start()
    for copy in early + late:
        copy.wait()


def solution(mesh):
    def body(x, wg, wu, wd):
        r, d = x.shape
        kd, ff = wg.shape
        bf, f32 = jnp.bfloat16, jnp.float32
        any_ = pl.BlockSpec(memory_space=pl.ANY)
        vmem = pl.BlockSpec(memory_space=pltpu.VMEM)
        nb = len(BLOCKS)
        nw = -(-ff // WC)
        shapes = [(nb, M, d), (nb + 2, M, d), (2, M, d), (r // C, C, d), (r // C, C, d), (kd, ff), (kd, ff), wd.shape]
        dma = pltpu.SemaphoreType.DMA
        params = dict(has_side_effects=True, vmem_limit_bytes=32 * 2**20)
        xv, acc, *_ = pl.pallas_call(
            kernel,
            out_shape=[pltpu.VMEM((M, d), bf), pltpu.VMEM((M, d), f32)] + [jax.ShapeDtypeStruct(s, bf) for s in shapes],
            in_specs=[any_] * 4,
            out_specs=[vmem] * 2 + [any_] * len(shapes),
            scratch_shapes=[
                pltpu.VMEM((2, d, FT), bf), pltpu.VMEM((2, d, FT), bf), pltpu.VMEM((2, FT, d), bf),
                pltpu.VMEM((M, FT), bf), pltpu.VMEM((2, S, d), bf), pltpu.VMEM((2, S, d), bf),
                dma((nb, M // C)), dma((nb, M // C)), dma((nb, M // C)), dma((nb, M // C)),
                dma((3, nw)), dma((3, nw)), dma((2, 6)), dma((M // C,)), dma((2,)), dma((2,)), dma((6,)),
            ],
            compiler_params=pltpu.CompilerParams(collective_id=0, **params),
        )(x, wg, wu, wd)
        return pl.pallas_call(
            write,
            out_shape=jax.ShapeDtypeStruct((r, d), bf),
            in_specs=[vmem] * 2,
            out_specs=any_,
            scratch_shapes=[pltpu.VMEM((M, d), bf), dma((10,))],
            compiler_params=pltpu.CompilerParams(vmem_limit_bytes=16 * 2**20),
        )(xv, acc)

    return jax.shard_map(body, mesh=mesh, in_specs=(P(("dp", "tp"), None), P("dp", "tp"), P("dp", "tp"), P("tp", "dp")), out_specs=P(("dp", "tp"), None), check_vma=False)
```

```python
import jax
import jax.numpy as jnp
from jax import lax
from jax.experimental import pallas as pl
from jax.experimental.pallas import tpu as pltpu
from jax.sharding import PartitionSpec as P

MESH = pl.DeviceIdType.MESH
M = 1024
FT = 256
NF = 14
C = 256
WC = 384
NC = 1280
MS = 512
R = 32
L0 = 6
V0 = 11

O1, O2, N1, N2 = range(4)
MINE, YS, LATE = range(3)
JOBS = (
    (O1, MINE, 0, 14, 1, 1, "zs"),
    (O2, MINE, 0, 14, 1, 1, "zs"),
    (N1, MINE, 0, 14, 1, 1, "z-"),
    (N1, YS, 0, 5, 1, 1, "k-"),
    (O1, YS, 0, 5, 1, 0, "k-"),
    (O2, YS, 0, 5, 1, 0, "k-"),
    (N1, YS, 5, 1, 1, 1, "kr"),
    (N2, MINE, 0, 14, 1, 1, "z-"),
    (N2, YS, 0, 7, 1, 1, "k-"),
    (N1, YS, 6, 2, 1, 0, "k-"),
    (O1, YS, 5, 3, 1, 0, "k-"),
    (O2, YS, 5, 3, 1, 0, "k-"),
    (N2, YS, 7, 2, 1, 1, "kr"),
    (O1, YS, 0, 8, 0, 1, "ls"),
    (O2, YS, 0, 8, 0, 1, "ls"),
    (N1, YS, 8, 2, 1, 0, "k-"),
    (N2, YS, 9, 1, 1, 0, "k-"),
    (O1, YS, 8, 2, 1, 0, "k-"),
    (O2, YS, 8, 2, 1, 0, "k-"),
    (N1, YS, 10, 1, 1, 0, "k-"),
    (O1, YS, 10, 1, 1, 0, "k-"),
    (O2, YS, 10, 1, 1, 0, "k-"),
    (O1, YS, 8, 3, 0, 1, "l-"),
    (O1, LATE, 6, 2, 0, 1, "ks"),
    (N1, YS, 11, 1, 1, 0, "k-"),
    (O1, YS, 11, 1, 1, 0, "k-"),
    (O2, YS, 11, 1, 1, 0, "k-"),
    (O2, YS, 8, 4, 0, 1, "ls"),
    (N1, YS, 12, 1, 1, 0, "k-"),
    (O1, YS, 12, 1, 1, 0, "k-"),
    (O2, YS, 12, 1, 1, 0, "k-"),
    (N1, YS, 13, 1, 1, 0, "k-"),
    (N2, YS, 10, 4, 1, 0, "k-"),
    (O1, YS, 13, 1, 1, 0, "k-"),
    (O2, YS, 13, 1, 1, 0, "k-"),
    (O1, YS, 11, 3, 0, 1, "l-"),
    (O1, LATE, 8, 6, 0, 1, "k-"),
    (O2, YS, 12, 2, 0, 1, "l-"),
    (O2, LATE, 9, 5, 0, 1, "k-"),
)
NJ = len(JOBS)
AHEAD = {2: (0, 1), 3: (2, 3), 8: (6,)}
FORWARD = {9: (6, 7), 15: (8, 9), 19: (10,)}
TURN = 8
SPREAD = {17: (6, 7), 32: (8, 9), 36: (10, 11, 12, 13)}
FINAL = (22, 27)
LEAVE = 36


def plan():
    slots, new, ahead, fresh = [], [], [], []
    group, last, seen, firsts = -1, None, 0, []
    for j, (rows, src, f0, n, s1, s2, _) in enumerate(JOBS):
        starts = bool(s1 and rows != last)
        if starts:
            group, last = group + 1, rows
            firsts.append(j)
        slots.append(max(group, 0) % 2)
        new.append(int(starts))
        top = f0 + n
        fresh.append(max(seen, f0) if src == YS and s1 and top > seen else NF)
        if src == YS and s1:
            seen = max(seen, top)
    late = 2
    load = [-1] * NJ
    for a, b in zip(firsts, firsts[1:]):
        load[b if b == late else a] = JOBS[b][0]
    return slots, new, load, fresh


SLOT, NEW, LOAD, FRESH = plan()


def kernel(x, wg, wu, wd, xv, acc, gn, pg, pu, pd, yg, yu, yd, ld, xd, ho, hs, hr, sv, prod, part,
           gv, uv, dv, hv,
           y_send, y_recv, d_send, d_recv, w_send, w_recv, l_send, l_recv, e_send, e_recv, n_send, n_recv,
           r_send, r_recv, h_send, h_recv, t_sem, w_load, x_load, s_sem, h_sem, o_sem):
    tp, dp = lax.axis_index("tp"), lax.axis_index("dp")
    to_x = {"tp": tp + 1 - 2 * (tp % 2)}
    to_y = {"tp": tp + 2 - 4 * (tp // 2)}
    to_core = {"dp": 1 - dp}
    kd, ff = wg.shape
    dc = wd.shape[1]
    f32, bf16 = jnp.float32, jnp.bfloat16
    last = (NF - 1) * FT
    own_rows = x.shape[0]

    barrier = pltpu.get_barrier_semaphore()
    for who in (to_x, to_y, to_core):
        pl.semaphore_signal(barrier, inc=1, device_id=who, device_id_type=MESH)
    pl.semaphore_wait(barrier, 3)

    def remote(src, dst, send, recv, who):
        return pltpu.make_async_remote_copy(
            src_ref=src, dst_ref=dst, send_sem=send, recv_sem=recv, device_id=who, device_id_type=MESH)

    def pick(values, j):
        got = jnp.int32(values[0])
        for k, v in enumerate(values):
            if v != values[0]:
                got = jnp.where(j == k, v, got)
        return got

    def col(t):
        return t * FT if isinstance(t, int) else pl.multiple_of(t * FT, FT)

    def tokens(q):
        return remote(x.at[pl.ds(q * C, C)], gn.at[q // (M // C), pl.ds(q % (M // C) * C, C)], n_send.at[q], n_recv.at[q], to_x)

    def mine(k, c):
        at = c * WC if isinstance(c, int) else pl.multiple_of(c * WC, WC)
        ref, peer = ((wg, pg), (wu, pu), (wd, pd))[k]
        ix = (pl.ds(at, WC),) if k == 2 else (slice(None), pl.ds(at, WC))
        return remote(ref.at[ix], peer.at[ix], w_send.at[k, c], w_recv.at[k, c], to_core)

    def y_tile(k, t, width):
        ref, mirror = ((wg, yg), (wu, yu), (wd, yd))[k]
        span = pl.ds(col(t), width)
        return ref.at[(span,) if k == 2 else (slice(None), span)], mirror.at[(0, span) if k == 2 else (0, slice(None), span)], mirror.at[(1, span) if k == 2 else (1, slice(None), span)]

    def along_y(k, t, width=FT):
        src, dst, _ = y_tile(k, t, width)
        return remote(src, dst, y_send.at[k, t], y_recv.at[k, t], to_y)

    def across(k, t, width=FT):
        _, src, dst = y_tile(k, t, width)
        return remote(src, dst, d_send.at[k, t], d_recv.at[k, t], to_core)

    def width_of(t):
        return ff - last if t == NF - 1 else FT

    def late_rows(t):
        return pl.ds(col(t - L0), width_of(t) if isinstance(t, int) else FT)

    def late_send(t):
        if t < V0:
            return remote(yd.at[0, pl.ds(col(t), FT)], ld.at[0, late_rows(t)], l_send.at[t - L0], l_recv.at[t - L0], to_x)
        return remote(xd.at[pl.ds(col(t - V0), width_of(t))], ld.at[0, late_rows(t)], l_send.at[t - L0], l_recv.at[t - L0], to_y)

    def late_across(t, rows):
        return remote(ld.at[0, rows], ld.at[1, rows], e_send.at[t - L0], e_recv.at[t - L0], to_core)

    def turn():
        return remote(wd.at[pl.ds(V0 * FT, ff - V0 * FT)], xd, t_sem.at[0], t_sem.at[1], to_x)

    def hidden(k, t, end=False):
        at = (k, t, slice(None), pl.ds(NF * FT - ff, ff - last)) if end else (k, t)
        return remote(hs.at[at], hr.at[at], h_send.at[k, t], h_recv.at[k, t], to_x)

    def products(k, q):
        rows = pl.ds(q * C, C)
        return remote(prod.at[k, rows], part.at[k, rows], r_send.at[k, q], r_recv.at[k, q], to_x)

    for q in range(own_rows // C):
        tokens(q).start()
    turn().start()
    for t in range(NF):
        for k in range(3):
            along_y(k, t, width_of(t)).start()
    for c in range(ff // WC):
        for k in range(3):
            mine(k, c).start()

    def tile_at(f):
        return pl.multiple_of(lax.min(f * FT, ff - FT), 128)

    def halves(extent):
        return [pl.ds(pl.multiple_of(core * extent, 128), extent) for core in (dp, 1 - dp)]

    def load_first(slot, f, src):
        at = tile_at(f)
        copies = []
        for k, (pair, dst) in enumerate((((wg, pg) if src == MINE else (yg.at[0], yg.at[1]), gv),
                                         ((wu, pu) if src == MINE else (yu.at[0], yu.at[1]), uv))):
            for m, (ref, rows) in enumerate(zip(pair, halves(kd))):
                copies.append(pltpu.make_async_copy(ref.at[:, pl.ds(at, FT)], dst.at[slot, rows], w_load.at[slot, 2 * k + m]))
        return copies

    def load_second(slot, f, src):
        at = tile_at(f) if src != LATE else pl.multiple_of(tile_at(f) - L0 * FT, 128)
        pair = {MINE: (wd, pd), YS: (yd.at[0], yd.at[1]), LATE: (ld.at[0], ld.at[1])}[src]
        return [pltpu.make_async_copy(ref.at[pl.ds(at, FT)], dv.at[slot, :, cols], w_load.at[slot, 4 + m])
                for m, (ref, cols) in enumerate(zip(pair, halves(dc)))]

    def load_h(slot, rows, f, src, end=False):
        cols = pl.ds(NF * FT - ff, ff - last) if end else slice(None)
        return pltpu.make_async_copy((hr if src == LATE else ho).at[rows, f, :, cols], hv.at[slot, :, cols], w_load.at[slot, 6])

    def load_x(rows, slot):
        own = pltpu.make_async_copy(x.at[pl.ds(pl.multiple_of(lax.min(rows, 1) * M, M), M)], xv.at[slot], x_load.at[slot])
        other = pltpu.make_async_copy(gn.at[lax.max(rows - 2, 0)], xv.at[slot], x_load.at[slot])
        return own, other

    def start_x(rows, slot):
        @pl.when(rows < N1)
        def _():
            load_x(rows, slot)[0].start()

        @pl.when(rows >= N1)
        def _():
            load_x(rows, slot)[1].start()

    def send_across(t, wait_first=True):
        for k in range(3):
            along_y(k, t, width_of(t)).wait_recv()
        for k in range(3):
            across(k, t, width_of(t)).start()

    def prefetch(slot, rows, src, f, first, second, fresh):
        @pl.when((src == MINE) & (rows == O1) & (f % 3 != 2) & (f < NF - 1))
        def _():
            for k in range(3):
                mine(k, (2 * f + 2) // 3).wait_recv()

        is_new = (src == YS) & (first == 1) & (f >= fresh)
        early = [t for ts in AHEAD.values() for t in ts]
        to_send = is_new
        for t in early:
            to_send = to_send & (f != t)

        @pl.when(to_send & (f < NF - 1))
        def _():
            for k in range(3):
                along_y(k, f).wait_recv()
            for k in range(3):
                across(k, f).start()

        @pl.when(is_new & (f < NF - 1))
        def _():
            for k in range(3):
                across(k, f).wait_recv()

        @pl.when(is_new & (f == NF - 1))
        def _():
            send_across(NF - 1)
            for k in range(3):
                across(k, NF - 1, width_of(NF - 1)).wait_recv()

        @pl.when((src == LATE) & (f < NF - 1))
        def _():
            hidden(rows, f).wait_recv()

        @pl.when((src == LATE) & (f == NF - 1))
        def _():
            hidden(rows, NF - 1, True).wait_recv()
            hv[slot, :, pl.ds(0, NF * FT - ff)] = jnp.zeros((M, NF * FT - ff), bf16)
            load_h(slot, rows, NF - 1, LATE, True).start()

        @pl.when((src == LATE) & (rows == O1) & (f < NF - 1))
        def _():
            late_across(f, late_rows(f)).wait_recv()

        @pl.when((src == LATE) & (rows == O1) & (f == NF - 1))
        def _():
            late_across(NF - 1, late_rows(NF - 1)).wait_recv()

        for value in (MINE, YS):
            @pl.when((first == 1) & (src == value))
            def _():
                for copy in load_first(slot, f, value):
                    copy.start()
        for value in (MINE, YS, LATE):
            @pl.when((second == 1) & (src == value))
            def _():
                for copy in load_second(slot, f, value):
                    copy.start()
        for value in (YS, LATE):
            @pl.when((first == 0) & (src == value) & ((src == YS) | (f < NF - 1)))
            def _():
                load_h(slot, rows, f, value).start()

    def store_h(slot, rows, f):
        return (pltpu.make_async_copy(hv.at[slot], ho.at[lax.min(rows, 1), f], h_sem.at[slot]),
                pltpu.make_async_copy(hv.at[slot], hs.at[lax.max(rows - 2, 0), f], h_sem.at[slot]))

    def swap(k, out):
        return pltpu.make_async_copy(acc, sv.at[k], s_sem) if out else pltpu.make_async_copy(sv.at[k], acc, s_sem)

    def store(k, q, slot):
        rows = pl.ds(q * C, C)
        return pltpu.make_async_copy(xv.at[slot, rows], prod.at[k, rows], o_sem.at[q])

    start_x(jnp.int32(O1), 0)
    prefetch(0, jnp.int32(O1), jnp.int32(MINE), jnp.int32(0), jnp.int32(1), jnp.int32(1), jnp.int32(NF))

    columns = [[job[i] for job in JOBS] for i in range(6)]
    modes = [job[6] for job in JOBS]

    def job(j, step0):
        rows, src, f0, n, first, second = [pick(c, j) for c in columns]
        after = lax.min(j + 1, NJ - 1)
        rows_n, src_n, f0_n, _, first_n, second_n = [pick(c, after) for c in columns]
        fresh, fresh_n = pick(FRESH, j), pick(FRESH, after)
        slot_x = pick(SLOT, j)
        load_n = pick(LOAD, j)
        is_h = (first == 1) & (second == 0)
        before = lax.max(j - 1, 0)
        own_h_before = pick([int(a[4] and not a[5] and a[0] < N1) for a in JOBS], before)

        for at, tiles in AHEAD.items():
            @pl.when(j == at)
            def _():
                for t in tiles:
                    send_across(t)
        @pl.when(j == 2)
        def _():
            for q in range(M // C):
                tokens(q).wait_recv()
        @pl.when(j == 6)
        def _():
            for q in range(M // C, own_rows // C):
                tokens(q).wait_recv()
        @pl.when(j == TURN)
        def _():
            turn().wait_recv()
            for t in range(V0, NF):
                late_send(t).start()
        for at, tiles in SPREAD.items():
            @pl.when(j == at)
            def _():
                for t in tiles:
                    late_send(t).wait_recv()
                for t in tiles:
                    late_across(t, late_rows(t)).start()

        new = pick(NEW, j) == 1
        @pl.when(j == 2)
        def _():
            start_x(rows, slot_x)

        @pl.when(new)
        def _():
            load_x(rows, slot_x)[0].wait()

        @pl.when((load_n >= 0) & (j != 2))
        def _():
            start_x(load_n, 1 - slot_x)

        @pl.when(j == 2)
        def _():
            start_x(pick([JOBS[4][0]], j), 1 - slot_x)

        @pl.when(pick([int(m[0] == "z") for m in modes], j) == 1)
        def _():
            @pl.loop(0, M // R)
            def _(r):
                acc[pl.ds(pl.multiple_of(r * R, R), R)] = jnp.zeros((R, acc.shape[1]), f32)

        @pl.when(pick([int(m[0] == "l") for m in modes], j) == 1)
        def _():
            swap(rows, False).start()
            swap(rows, False).wait()

        for k, at_job in enumerate(FINAL):
            @pl.when(j == at_job)
            def _():
                for q in range(M // C):
                    products(k, q).wait_recv()
                for ref in (x.at[pl.ds(k * M, M)], part.at[k]):
                    copy = pltpu.make_async_copy(ref, xv.at[slot_x], x_load.at[slot_x])
                    copy.start()
                    copy.wait()

                    @pl.loop(0, M // R)
                    def _(r):
                        at = pl.ds(pl.multiple_of(r * R, R), R)
                        acc[at] = acc[at] + xv[slot_x, at].astype(f32)

        def step(i, _):
            f = f0 + i
            slot = (step0 + i) % 2
            ends = i + 1 == n

            @pl.when(jnp.where(i == 0, own_h_before == 1, is_h))
            def _():
                store_h(1 - slot, rows, f)[0].wait()

            @pl.when(first == 1)
            def _():
                for copy in load_first(slot, f, MINE):
                    copy.wait()

            @pl.when(second == 1)
            def _():
                for copy in load_second(slot, f, MINE):
                    copy.wait()

            half_h = (src == LATE) & (f == NF - 1)

            @pl.when((first == 0) & jnp.logical_not(half_h))
            def _():
                load_h(slot, rows, f, YS).wait()

            @pl.when(half_h)
            def _():
                load_h(slot, rows, f, YS, True).wait()

            @pl.when(jnp.logical_not(ends & (j == NJ - 1)))
            def _():
                prefetch(1 - slot, jnp.where(ends, rows_n, rows), jnp.where(ends, src_n, src), jnp.where(ends, f0_n, f + 1),
                         jnp.where(ends, first_n, first), jnp.where(ends, second_n, second), jnp.where(ends, fresh_n, fresh))

            @pl.when(first == 1)
            def _():
                skip = lax.max(f * FT - (ff - FT), 0)
                own = lax.broadcasted_iota(jnp.int32, (MS, FT), 1) >= skip
                for r in range(0, M, MS):
                    at = slice(r, r + MS)
                    a = jnp.dot(xv[slot_x, at], gv[slot], preferred_element_type=f32)
                    b = jnp.dot(xv[slot_x, at], uv[slot], preferred_element_type=f32)
                    hv[slot, at] = jnp.where(own, a * jax.nn.sigmoid(a) * b, 0.0).astype(bf16)

            @pl.when(second == 1)
            def _():
                for c in range(0, acc.shape[1], NC):
                    cols = slice(c, c + NC)
                    acc[:, cols] += jnp.dot(hv[slot], dv[slot, :, cols], preferred_element_type=f32)

            @pl.when(is_h & (rows < N1))
            def _():
                store_h(slot, rows, f)[0].start()

            @pl.when(is_h & (rows >= N1))
            def _():
                store_h(slot, rows, f)[1].start()
            return 0

        lax.fori_loop(0, n, step, 0)

        @pl.when(is_h & (rows >= N1))
        def _():
            store_h((step0 + n - 1) % 2, rows, f0)[1].wait()

            @pl.loop(0, n)
            def _(i):
                @pl.when(f0 + i < NF - 1)
                def _():
                    hidden(rows - 2, f0 + i).start()

                @pl.when(f0 + i == NF - 1)
                def _():
                    hidden(rows - 2, NF - 1, True).start()

        for at, tiles in FORWARD.items():
            @pl.when(j == at)
            def _():
                for t in tiles:
                    late_send(t).start()

        @pl.when(pick([int(m[1] == "s") for m in modes], j) == 1)
        def _():
            swap(rows, True).start()
            swap(rows, True).wait()

        @pl.when(pick([int(m[1] == "r") for m in modes], j) == 1)
        def _():
            for q in range(M // C):
                @pl.loop(0, C // R)
                def _(r):
                    at = pl.ds(pl.multiple_of(q * C + r * R, R), R)
                    xv[slot_x, at] = acc[at].astype(bf16)
                store(rows - 2, q, slot_x).start()
            for q in range(M // C):
                store(rows - 2, q, slot_x).wait()
                products(rows - 2, q).start()

        @pl.when(j == LEAVE)
        def _():
            @pl.loop(0, M // R)
            def _(r):
                at = pl.ds(pl.multiple_of(r * R, R), R)
                xv[0, at] = acc[at].astype(bf16)
        return step0 + n

    lax.fori_loop(0, NJ, job, jnp.int32(0))

    for q in range(own_rows // C):
        tokens(q).wait_send()
    turn().wait_send()
    for t in range(NF):
        for k in range(3):
            along_y(k, t, width_of(t)).wait_send()
            across(k, t, width_of(t)).wait_send()
    for c in range(ff // WC):
        for k in range(3):
            mine(k, c).wait_send()
    for t in range(L0, NF):
        late_send(t).wait_send()
        late_across(t, late_rows(t)).wait_send()
    for k in range(2):
        for q in range(M // C):
            products(k, q).wait_send()
    for rows, src, f0, n, first, second, _ in JOBS:
        if rows >= N1 and not second:
            for t in range(f0, f0 + n):
                hidden(rows - 2, t, t == NF - 1).wait_send()


def write(xv, acc, out, yv, sem):
    step = 128
    early = pltpu.make_async_copy(xv.at[0], out.at[pl.ds(0, M)], sem.at[0])
    early.start()
    late = [pltpu.make_async_copy(yv.at[pl.ds(k * step, step)], out.at[pl.ds(M + k * step, step)], sem.at[1 + k])
            for k in range(M // step)]
    for k, copy in enumerate(late):
        @pl.loop(0, step // R)
        def _(r):
            at = pl.ds(pl.multiple_of(k * step + r * R, R), R)
            yv[at] = acc[at].astype(jnp.bfloat16)
        copy.start()
    early.wait()
    for copy in late:
        copy.wait()


def solution(mesh):
    def body(x, wg, wu, wd):
        r, d = x.shape
        kd, ff = wg.shape
        dc = wd.shape[1]
        bf, f32 = jnp.bfloat16, jnp.float32
        any_ = pl.BlockSpec(memory_space=pl.ANY)
        vmem = pl.BlockSpec(memory_space=pltpu.VMEM)
        nh = (2, NF, M, FT)
        shapes = [(2, M, d), (kd, ff), (kd, ff), (ff, dc), (2, kd, ff), (2, kd, ff), (2, ff, dc),
                  (2, ff - L0 * FT, dc), (ff - V0 * FT, dc), nh, nh, nh]
        dma = pltpu.SemaphoreType.DMA
        nl, nn, nw = NF - L0, r // C, ff // WC
        work = [jax.ShapeDtypeStruct(s, bf) for s in shapes] + [
            jax.ShapeDtypeStruct((2, M, d), f32), jax.ShapeDtypeStruct((2, M, d), bf), jax.ShapeDtypeStruct((2, M, d), bf)]
        xv, acc, *_ = pl.pallas_call(
            kernel,
            out_shape=[pltpu.VMEM((2, M, d), bf), pltpu.VMEM((M, d), f32)] + work,
            in_specs=[any_] * 4,
            out_specs=[vmem] * 2 + [any_] * len(work),
            scratch_shapes=[
                pltpu.VMEM((2, d, FT), bf), pltpu.VMEM((2, d, FT), bf), pltpu.VMEM((2, FT, d), bf),
                pltpu.VMEM((2, M, FT), bf),
                dma((3, NF)), dma((3, NF)), dma((3, NF)), dma((3, NF)), dma((3, nw)), dma((3, nw)),
                dma((nl,)), dma((nl,)), dma((nl,)), dma((nl,)), dma((nn,)), dma((nn,)),
                dma((2, M // C)), dma((2, M // C)), dma((2, NF)), dma((2, NF)), dma((2,)),
                dma((2, 7)), dma((2,)), dma, dma((2,)), dma((M // C,)),
            ],
            compiler_params=pltpu.CompilerParams(collective_id=0, has_side_effects=True, vmem_limit_bytes=23 * 2**20),
        )(x, wg, wu, wd)
        return pl.pallas_call(
            write,
            out_shape=jax.ShapeDtypeStruct((r, d), bf),
            in_specs=[vmem] * 2,
            out_specs=any_,
            scratch_shapes=[pltpu.VMEM((M, d), bf), dma((9,))],
            compiler_params=pltpu.CompilerParams(vmem_limit_bytes=12 * 2**20),
        )(xv, acc)

    return jax.shard_map(body, mesh=mesh, in_specs=(P(("dp", "tp"), None), P("dp", "tp"), P("dp", "tp"), P("tp", "dp")), out_specs=P(("dp", "tp"), None), check_vma=False)
```

```python
import jax
import jax.numpy as jnp
from jax import lax
from jax.experimental import pallas as pl
from jax.experimental.pallas import tpu as pltpu
from jax.sharding import PartitionSpec as P

MESH = pl.DeviceIdType.MESH
M = 1024
FT = 256
NF = 14
C = 256
WC = 384
NC = 1280
MS = 512
R = 32
L0 = 6
TURN_ROW = 2688
PIECES = ((1536, 256), (1792, 256), (2048, 256), (2304, 256), (2560, 128), (2688, 128), (2816, 256), (3072, 256), (3328, 128))

O1, O2, N1, N2 = range(4)
MINE, YS, LATE = range(3)
JOBS = (
    (O1, MINE, 0, 14, 1, 1, "zs"),
    (O2, MINE, 0, 14, 1, 1, "zs"),
    (N1, MINE, 0, 14, 1, 1, "z-"),
    (N1, YS, 0, 5, 1, 1, "k-"),
    (O1, YS, 0, 5, 1, 0, "k-"),
    (O2, YS, 0, 5, 1, 0, "k-"),
    (N1, YS, 5, 1, 1, 1, "kr"),
    (N2, MINE, 0, 14, 1, 1, "z-"),
    (N2, YS, 0, 7, 1, 1, "k-"),
    (N1, YS, 6, 2, 1, 0, "k-"),
    (O1, YS, 5, 3, 1, 0, "k-"),
    (O2, YS, 5, 3, 1, 0, "k-"),
    (N2, YS, 7, 2, 1, 1, "kr"),
    (O1, YS, 0, 8, 0, 1, "ls"),
    (O2, YS, 0, 8, 0, 1, "ls"),
    (N1, YS, 8, 2, 1, 0, "k-"),
    (N2, YS, 9, 1, 1, 0, "k-"),
    (O1, YS, 8, 2, 1, 0, "k-"),
    (O2, YS, 8, 2, 1, 0, "k-"),
    (N1, YS, 10, 1, 1, 0, "k-"),
    (O1, YS, 10, 1, 1, 0, "k-"),
    (O2, YS, 10, 1, 1, 0, "k-"),
    (N2, YS, 10, 1, 1, 0, "k-"),
    (O1, YS, 8, 3, 0, 1, "l-"),
    (O1, LATE, 6, 2, 0, 1, "ks"),
    (N1, YS, 11, 1, 1, 0, "k-"),
    (O1, YS, 11, 1, 1, 0, "k-"),
    (O2, YS, 11, 1, 1, 0, "k-"),
    (N2, YS, 11, 1, 1, 0, "k-"),
    (O2, YS, 8, 4, 0, 1, "lh"),
    (N1, YS, 12, 1, 1, 0, "k-"),
    (N2, YS, 12, 1, 1, 0, "k-"),
    (O1, YS, 12, 1, 1, 0, "k-"),
    (O2, YS, 12, 1, 1, 0, "k-"),
    (O1, YS, 11, 2, 0, 1, "l-"),
    (N2, YS, 13, 1, 1, 0, "k-"),
    (N1, YS, 13, 1, 1, 0, "k-"),
    (O1, YS, 13, 1, 1, 0, "k-"),
    (O2, YS, 13, 1, 1, 0, "k-"),
    (O1, YS, 13, 1, 0, 1, "k-"),
    (O1, LATE, 8, 2, 0, 1, "k-"),
    (O1, LATE, 10, 2, 0, 1, "kv"),
    (O2, YS, 12, 2, 0, 1, "h-"),
    (O2, LATE, 9, 3, 0, 1, "k-"),
    (O2, LATE, 12, 1, 0, 1, "k-"),
    (O2, LATE, 13, 1, 0, 1, "k-"),
    (O1, LATE, 12, 2, 0, 1, "v-"),
)
NJ = len(JOBS)
AHEAD = {2: (0, 1), 3: (2, 3), 8: (6,)}
FORWARD = {9: (0, 1), 15: (2, 3), 19: (4,)}
SENDS = {9: ((0, 6), (0, 7)), 15: ((0, 8), (0, 9)), 16: ((1, 9),), 19: ((0, 10),), 25: ((0, 11),), 28: ((1, 10), (1, 11)),
         31: ((1, 12),), 35: ((1, 13),), 36: ((0, 12), (0, 13))}
TURN = 8
SPREAD = {17: (0, 1), 35: (2, 3), 40: (4, 5, 6), 43: (7,), 44: (8,)}
FINAL = (23, 29)
FETCH = 39
LEAVE = 45
PATIENT = (43, 44, 45)
SECOND = 12


def plan():
    slots, new, ahead, fresh = [], [], [], []
    group, last, seen, firsts = -1, None, 0, []
    for j, (rows, src, f0, n, s1, s2, _) in enumerate(JOBS):
        starts = bool(s1 and rows != last)
        if starts:
            group, last = group + 1, rows
            firsts.append(j)
        slots.append(max(group, 0) % 2)
        new.append(int(starts))
        top = f0 + n
        fresh.append(max(seen, f0) if src == YS and s1 and top > seen else NF)
        if src == YS and s1:
            seen = max(seen, top)
    late = 2
    load = [-1] * NJ
    for a, b in zip(firsts, firsts[1:]):
        load[b if b == late else a] = JOBS[b][0]
    return slots, new, load, fresh


SLOT, NEW, LOAD, FRESH = plan()


def spot(b, gv, uv):
    per = gv.shape[1] // M
    return (gv, uv)[b // (2 * per)], b // per % 2, b % per * M


def kernel(x, wg, wu, wd, gv, uv, acc, gn, pg, pu, pd, yg, yu, yd, ld, xd, ho, hs, hr, sv, sh, prod, part,
           xv, dv, hv,
           y_send, y_recv, d_send, d_recv, w_send, w_recv, l_send, l_recv, e_send, e_recv, n_send, n_recv,
           r_send, r_recv, h_send, h_recv, t_sem, w_load, x_load, s_sem, h_sem, o_sem):
    tp, dp = lax.axis_index("tp"), lax.axis_index("dp")
    to_x = {"tp": tp + 1 - 2 * (tp % 2)}
    to_y = {"tp": tp + 2 - 4 * (tp // 2)}
    to_core = {"dp": 1 - dp}
    kd, ff = wg.shape
    dc = wd.shape[1]
    f32, bf16 = jnp.float32, jnp.bfloat16
    last = (NF - 1) * FT
    own_rows = x.shape[0]

    barrier = pltpu.get_barrier_semaphore()
    for who in (to_x, to_y, to_core):
        pl.semaphore_signal(barrier, inc=1, device_id=who, device_id_type=MESH)
    pl.semaphore_wait(barrier, 3)

    def remote(src, dst, send, recv, who):
        return pltpu.make_async_remote_copy(
            src_ref=src, dst_ref=dst, send_sem=send, recv_sem=recv, device_id=who, device_id_type=MESH)

    def pick(values, j):
        got = jnp.int32(values[0])
        for k, v in enumerate(values):
            if v != values[0]:
                got = jnp.where(j == k, v, got)
        return got

    def col(t):
        return t * FT if isinstance(t, int) else pl.multiple_of(t * FT, FT)

    def tokens(q):
        return remote(x.at[pl.ds(q * C, C)], gn.at[q // (M // C), pl.ds(q % (M // C) * C, C)], n_send.at[q], n_recv.at[q], to_x)

    def mine(k, c):
        at = c * WC if isinstance(c, int) else pl.multiple_of(c * WC, WC)
        ref, peer = ((wg, pg), (wu, pu), (wd, pd))[k]
        ix = (pl.ds(at, WC),) if k == 2 else (slice(None), pl.ds(at, WC))
        return remote(ref.at[ix], peer.at[ix], w_send.at[k, c], w_recv.at[k, c], to_core)

    def y_tile(k, t, width):
        ref, mirror = ((wg, yg), (wu, yu), (wd, yd))[k]
        span = pl.ds(col(t), width)
        return ref.at[(span,) if k == 2 else (slice(None), span)], mirror.at[(0, span) if k == 2 else (0, slice(None), span)], mirror.at[(1, span) if k == 2 else (1, slice(None), span)]

    def along_y(k, t, width=FT):
        src, dst, _ = y_tile(k, t, width)
        return remote(src, dst, y_send.at[k, t], y_recv.at[k, t], to_y)

    def across(k, t, width=FT):
        _, src, dst = y_tile(k, t, width)
        return remote(src, dst, d_send.at[k, t], d_recv.at[k, t], to_core)

    def width_of(t):
        return ff - last if t == NF - 1 else FT

    def late_send(p):
        row, n = PIECES[p]
        dst = ld.at[0, pl.ds(row - L0 * FT, n)]
        if row < TURN_ROW:
            return remote(yd.at[0, pl.ds(row, n)], dst, l_send.at[p], l_recv.at[p], to_x)
        return remote(xd.at[pl.ds(row - TURN_ROW, n)], dst, l_send.at[p], l_recv.at[p], to_y)

    def late_across(p):
        row, n = PIECES[p]
        at = pl.ds(row - L0 * FT, n)
        return remote(ld.at[0, at], ld.at[1, at], e_send.at[p], e_recv.at[p], to_core)

    def turn():
        return remote(wd.at[pl.ds(TURN_ROW, ff - TURN_ROW)], xd, t_sem.at[0], t_sem.at[1], to_x)

    def hidden(k, t, end=False):
        at = (k, t, slice(None), pl.ds(NF * FT - ff, ff - last)) if end else (k, t)
        return remote(hs.at[at], hr.at[at], h_send.at[k, t], h_recv.at[k, t], to_x)

    def products(k, q):
        rows = pl.ds(q * C, C)
        return remote(prod.at[k, rows], part.at[k, rows], r_send.at[k, q], r_recv.at[k, q], to_x)

    for q in range(own_rows // C):
        tokens(q).start()
    turn().start()
    for t in range(NF):
        for k in range(3):
            along_y(k, t, width_of(t)).start()
    for c in range(ff // WC):
        for k in range(3):
            mine(k, c).start()

    def tile_at(f):
        return pl.multiple_of(lax.min(f * FT, ff - FT), 128)

    def halves(extent):
        return [pl.ds(pl.multiple_of(core * extent, 128), extent) for core in (dp, 1 - dp)]

    def load_first(slot, f, src):
        at = tile_at(f)
        copies = []
        for k, (pair, dst) in enumerate((((wg, pg) if src == MINE else (yg.at[0], yg.at[1]), gv),
                                         ((wu, pu) if src == MINE else (yu.at[0], yu.at[1]), uv))):
            for m, (ref, rows) in enumerate(zip(pair, halves(kd))):
                copies.append(pltpu.make_async_copy(ref.at[:, pl.ds(at, FT)], dst.at[slot, rows], w_load.at[slot, 2 * k + m]))
        return copies

    def load_second(slot, f, src):
        at = tile_at(f) if src != LATE else pl.multiple_of(tile_at(f) - L0 * FT, 128)
        pair = {MINE: (wd, pd), YS: (yd.at[0], yd.at[1]), LATE: (ld.at[0], ld.at[1])}[src]
        return [pltpu.make_async_copy(ref.at[pl.ds(at, FT)], dv.at[slot, :, cols], w_load.at[slot, 4 + m])
                for m, (ref, cols) in enumerate(zip(pair, halves(dc)))]

    def load_h(slot, rows, f, src, end=False):
        cols = pl.ds(NF * FT - ff, ff - last) if end else slice(None)
        return pltpu.make_async_copy((hr if src == LATE else ho).at[rows, f, :, cols], hv.at[slot, :, cols], w_load.at[slot, 6])

    def load_x(rows, slot):
        own = pltpu.make_async_copy(x.at[pl.ds(pl.multiple_of(lax.min(rows, 1) * M, M), M)], xv.at[slot], x_load.at[slot])
        other = pltpu.make_async_copy(gn.at[lax.max(rows - 2, 0)], xv.at[slot], x_load.at[slot])
        return own, other

    def start_x(rows, slot):
        @pl.when(rows < N1)
        def _():
            load_x(rows, slot)[0].start()

        @pl.when(rows >= N1)
        def _():
            load_x(rows, slot)[1].start()

    def send_across(t, wait_first=True):
        for k in range(3):
            along_y(k, t, width_of(t)).wait_recv()
        for k in range(3):
            across(k, t, width_of(t)).start()

    def prefetch(slot, rows, src, f, first, second, fresh):
        @pl.when((src == MINE) & (rows == O1) & (f % 3 != 2) & (f < NF - 1))
        def _():
            for k in range(3):
                mine(k, (2 * f + 2) // 3).wait_recv()

        is_new = (src == YS) & (first == 1) & (f >= fresh)
        early = [t for ts in AHEAD.values() for t in ts]
        to_send = is_new
        for t in early:
            to_send = to_send & (f != t)

        @pl.when(to_send & (f < NF - 1))
        def _():
            for k in range(3):
                along_y(k, f).wait_recv()
            for k in range(3):
                across(k, f).start()

        @pl.when(is_new & (f < NF - 1))
        def _():
            for k in range(3):
                across(k, f).wait_recv()

        @pl.when(is_new & (f == NF - 1))
        def _():
            send_across(NF - 1)
            for k in range(3):
                across(k, NF - 1, width_of(NF - 1)).wait_recv()

        @pl.when((src == LATE) & (f < NF - 1))
        def _():
            hidden(rows, f).wait_recv()

        @pl.when((src == LATE) & (f == NF - 1))
        def _():
            hidden(rows, NF - 1, True).wait_recv()
            hv[slot, :, pl.ds(0, NF * FT - ff)] = jnp.zeros((M, NF * FT - ff), bf16)
            load_h(slot, rows, NF - 1, LATE, True).start()

        for t in range(L0, NF):
            @pl.when((src == LATE) & (rows == (O1 if t < SECOND else O2)) & (f == t))
            def _():
                for p, (row, _) in enumerate(PIECES):
                    if row // FT == t:
                        late_across(p).wait_recv()

        for value in (MINE, YS):
            @pl.when((first == 1) & (src == value))
            def _():
                for copy in load_first(slot, f, value):
                    copy.start()
        for value in (MINE, YS, LATE):
            @pl.when((second == 1) & (src == value))
            def _():
                for copy in load_second(slot, f, value):
                    copy.start()
        for value in (YS, LATE):
            @pl.when((first == 0) & (src == value) & ((src == YS) | (f < NF - 1)))
            def _():
                load_h(slot, rows, f, value).start()

    def store_h(slot, rows, f):
        return (pltpu.make_async_copy(hv.at[slot], ho.at[lax.min(rows, 1), f], h_sem.at[slot]),
                pltpu.make_async_copy(hv.at[slot], hs.at[lax.max(rows - 2, 0), f], h_sem.at[slot]))

    def swap(k, out):
        return pltpu.make_async_copy(acc, sv.at[k], s_sem) if out else pltpu.make_async_copy(sv.at[k], acc, s_sem)

    def store(k, q, slot):
        rows = pl.ds(q * C, C)
        return pltpu.make_async_copy(xv.at[slot, rows], prod.at[k, rows], o_sem.at[q])

    start_x(jnp.int32(O1), 0)
    prefetch(0, jnp.int32(O1), jnp.int32(MINE), jnp.int32(0), jnp.int32(1), jnp.int32(1), jnp.int32(NF))

    columns = [[job[i] for job in JOBS] for i in range(6)]
    modes = [job[6] for job in JOBS]

    def job(j, step0):
        rows, src, f0, n, first, second = [pick(c, j) for c in columns]
        after = lax.min(j + 1, NJ - 1)
        rows_n, src_n, f0_n, _, first_n, second_n = [pick(c, after) for c in columns]
        fresh, fresh_n = pick(FRESH, j), pick(FRESH, after)
        slot_x = pick(SLOT, j)

        def is_mode(at, what):
            return pick([int(m[at] == what) for m in modes], j) == 1
        load_n = pick(LOAD, j)
        is_h = (first == 1) & (second == 0)
        before = lax.max(j - 1, 0)
        own_h_before = pick([int(a[4] and not a[5] and a[0] < N1) for a in JOBS], before)

        for at, tiles in AHEAD.items():
            @pl.when(j == at)
            def _():
                for t in tiles:
                    send_across(t)
        @pl.when(j == 2)
        def _():
            for q in range(M // C):
                tokens(q).wait_recv()
        @pl.when(j == 6)
        def _():
            for q in range(M // C, own_rows // C):
                tokens(q).wait_recv()
        @pl.when(j == TURN)
        def _():
            turn().wait_recv()
            for p, (row, _) in enumerate(PIECES):
                if row >= TURN_ROW:
                    late_send(p).start()
        for at, ps in SPREAD.items():
            @pl.when(j == at)
            def _():
                for p in ps:
                    late_send(p).wait_recv()
                for p in ps:
                    late_across(p).start()

        new = pick(NEW, j) == 1
        @pl.when(j == 2)
        def _():
            start_x(rows, slot_x)

        @pl.when(new)
        def _():
            load_x(rows, slot_x)[0].wait()

        @pl.when((load_n >= 0) & (j != 2))
        def _():
            start_x(load_n, 1 - slot_x)

        @pl.when(j == 2)
        def _():
            start_x(pick([JOBS[4][0]], j), 1 - slot_x)

        @pl.when(is_mode(0, "z"))
        def _():
            @pl.loop(0, M // R)
            def _(r):
                acc[pl.ds(pl.multiple_of(r * R, R), R)] = jnp.zeros((R, acc.shape[1]), f32)

        @pl.when(is_mode(0, "l"))
        def _():
            swap(rows, False).start()
            swap(rows, False).wait()

        def to_rows(slot):
            @pl.loop(0, M // R)
            def _(r):
                at = pl.ds(pl.multiple_of(r * R, R), R)
                xv[slot, at] = acc[at].astype(bf16)

        def from_rows(slot):
            @pl.loop(0, M // R)
            def _(r):
                at = pl.ds(pl.multiple_of(r * R, R), R)
                acc[at] = xv[slot, at].astype(f32)

        @pl.when(j == FETCH)
        def _():
            pltpu.make_async_copy(sh, xv.at[1], x_load.at[1]).start()

        @pl.when(is_mode(0, "h"))
        def _():
            pltpu.make_async_copy(sh, xv.at[1], x_load.at[1]).wait()
            from_rows(1)

        @pl.when(is_mode(0, "v"))
        def _():
            from_rows(0)

        for k, at_job in enumerate(FINAL):
            @pl.when(j == at_job)
            def _():
                for q in range(M // C):
                    products(k, q).wait_recv()
                for ref in (x.at[pl.ds(k * M, M)], part.at[k]):
                    copy = pltpu.make_async_copy(ref, xv.at[slot_x], x_load.at[slot_x])
                    copy.start()
                    copy.wait()

                    @pl.loop(0, M // R)
                    def _(r):
                        at = pl.ds(pl.multiple_of(r * R, R), R)
                        acc[at] = acc[at] + xv[slot_x, at].astype(f32)

        def step(i, _):
            f = f0 + i
            slot = (step0 + i) % 2
            ends = i + 1 == n

            @pl.when(jnp.where(i == 0, own_h_before == 1, is_h))
            def _():
                store_h(1 - slot, rows, f)[0].wait()

            @pl.when(first == 1)
            def _():
                for copy in load_first(slot, f, MINE):
                    copy.wait()

            @pl.when(second == 1)
            def _():
                for copy in load_second(slot, f, MINE):
                    copy.wait()

            half_h = (src == LATE) & (f == NF - 1)

            @pl.when((first == 0) & jnp.logical_not(half_h))
            def _():
                load_h(slot, rows, f, YS).wait()

            @pl.when(half_h)
            def _():
                load_h(slot, rows, f, YS, True).wait()

            def load_next():
                prefetch(1 - slot, jnp.where(ends, rows_n, rows), jnp.where(ends, src_n, src), jnp.where(ends, f0_n, f + 1),
                         jnp.where(ends, first_n, first), jnp.where(ends, second_n, second), jnp.where(ends, fresh_n, fresh))

            patient = (j >= PATIENT[0]) & (j <= PATIENT[-1])
            pl.when(jnp.logical_not(patient | (ends & (j == NJ - 1))))(load_next)

            @pl.when(first == 1)
            def _():
                skip = lax.max(f * FT - (ff - FT), 0)
                own = lax.broadcasted_iota(jnp.int32, (MS, FT), 1) >= skip
                for r in range(0, M, MS):
                    at = slice(r, r + MS)
                    a = jnp.dot(xv[slot_x, at], gv[slot], preferred_element_type=f32)
                    b = jnp.dot(xv[slot_x, at], uv[slot], preferred_element_type=f32)
                    hv[slot, at] = jnp.where(own, a * jax.nn.sigmoid(a) * b, 0.0).astype(bf16)

            @pl.when(second == 1)
            def _():
                for c in range(0, acc.shape[1], NC):
                    cols = slice(c, c + NC)
                    acc[:, cols] += jnp.dot(hv[slot], dv[slot, :, cols], preferred_element_type=f32)

            pl.when(patient)(load_next)

            @pl.when(is_h & (rows < N1))
            def _():
                store_h(slot, rows, f)[0].start()

            @pl.when(is_h & (rows >= N1))
            def _():
                store_h(slot, rows, f)[1].start()
            return 0

        lax.fori_loop(0, n, step, 0)

        @pl.when(is_h & (rows >= N1))
        def _():
            store_h((step0 + n - 1) % 2, rows, f0)[1].wait()

        for at, pairs in SENDS.items():
            @pl.when(j == at)
            def _():
                for k, t in pairs:
                    hidden(k, t, t == NF - 1).start()

        for at, ps in FORWARD.items():
            @pl.when(j == at)
            def _():
                for p in ps:
                    late_send(p).start()

        @pl.when(is_mode(1, "s"))
        def _():
            swap(rows, True).start()
            swap(rows, True).wait()

        @pl.when(is_mode(1, "h"))
        def _():
            to_rows(slot_x)
            copy = pltpu.make_async_copy(xv.at[slot_x], sh, s_sem)
            copy.start()
            copy.wait()

        @pl.when(is_mode(1, "v"))
        def _():
            to_rows(0)

        @pl.when(is_mode(1, "r"))
        def _():
            for q in range(M // C):
                @pl.loop(0, C // R)
                def _(r):
                    at = pl.ds(pl.multiple_of(q * C + r * R, R), R)
                    xv[slot_x, at] = acc[at].astype(bf16)
                store(rows - 2, q, slot_x).start()
            for q in range(M // C):
                store(rows - 2, q, slot_x).wait()
                products(rows - 2, q).start()

        @pl.when(j == LEAVE)
        def _():
            @pl.loop(0, M // R)
            def _(r):
                for b in range(acc.shape[1] // FT):
                    buf, k, row = spot(b, gv, uv)
                    at = pl.ds(pl.multiple_of(r * R, R), R)
                    buf[k, pl.ds(pl.multiple_of(row + r * R, R), R)] = acc[at, b * FT:(b + 1) * FT].astype(bf16)
        return step0 + n

    lax.fori_loop(0, NJ, job, jnp.int32(0))

    for q in range(own_rows // C):
        tokens(q).wait_send()
    turn().wait_send()
    for t in range(NF):
        for k in range(3):
            along_y(k, t, width_of(t)).wait_send()
            across(k, t, width_of(t)).wait_send()
    for c in range(ff // WC):
        for k in range(3):
            mine(k, c).wait_send()
    for p in range(len(PIECES)):
        late_send(p).wait_send()
        late_across(p).wait_send()
    for k in range(2):
        for q in range(M // C):
            products(k, q).wait_send()
    for pairs in SENDS.values():
        for k, t in pairs:
            hidden(k, t, t == NF - 1).wait_send()


def write(gv, uv, acc, out, yv, sem):
    step = 128
    early, late = [], []
    for b in range(out.shape[1] // FT):
        buf, k, row = spot(b, gv, uv)
        early.append(pltpu.make_async_copy(buf.at[k, pl.ds(row, M)], out.at[pl.ds(M, M), pl.ds(b * FT, FT)], sem.at[b]))
    for k in range(M // step):
        late.append(pltpu.make_async_copy(yv.at[pl.ds(k * step, step)], out.at[pl.ds(k * step, step)], sem.at[len(early) + k]))
    for copy in early:
        copy.start()
    for k, copy in enumerate(late):
        @pl.loop(0, step // R)
        def _(r):
            at = pl.ds(pl.multiple_of(k * step + r * R, R), R)
            yv[at] = acc[at].astype(jnp.bfloat16)
        copy.start()
    for copy in early + late:
        copy.wait()


def solution(mesh):
    def body(x, wg, wu, wd):
        r, d = x.shape
        kd, ff = wg.shape
        dc = wd.shape[1]
        bf, f32 = jnp.bfloat16, jnp.float32
        any_ = pl.BlockSpec(memory_space=pl.ANY)
        vmem = pl.BlockSpec(memory_space=pltpu.VMEM)
        nh = (2, NF, M, FT)
        shapes = [(2, M, d), (kd, ff), (kd, ff), (ff, dc), (2, kd, ff), (2, kd, ff), (2, ff, dc),
                  (2, ff - L0 * FT, dc), (ff - TURN_ROW, dc), nh, nh, nh]
        dma = pltpu.SemaphoreType.DMA
        nl, nn, nw = len(PIECES), r // C, ff // WC
        work = [jax.ShapeDtypeStruct(s, bf) for s in shapes] + [
            jax.ShapeDtypeStruct((2, M, d), f32), jax.ShapeDtypeStruct((M, d), bf), jax.ShapeDtypeStruct((2, M, d), bf), jax.ShapeDtypeStruct((2, M, d), bf)]
        gv, uv, acc, *_ = pl.pallas_call(
            kernel,
            out_shape=[pltpu.VMEM((2, d, FT), bf)] * 2 + [pltpu.VMEM((M, d), f32)] + work,
            in_specs=[any_] * 4,
            out_specs=[vmem] * 3 + [any_] * len(work),
            scratch_shapes=[
                pltpu.VMEM((2, M, d), bf), pltpu.VMEM((2, FT, d), bf), pltpu.VMEM((2, M, FT), bf),
                dma((3, NF)), dma((3, NF)), dma((3, NF)), dma((3, NF)), dma((3, nw)), dma((3, nw)),
                dma((nl,)), dma((nl,)), dma((nl,)), dma((nl,)), dma((nn,)), dma((nn,)),
                dma((2, M // C)), dma((2, M // C)), dma((2, NF)), dma((2, NF)), dma((2,)),
                dma((2, 7)), dma((2,)), dma, dma((2,)), dma((M // C,)),
            ],
            compiler_params=pltpu.CompilerParams(collective_id=0, has_side_effects=True, vmem_limit_bytes=int(33.9 * 2**20)),
        )(x, wg, wu, wd)
        return pl.pallas_call(
            write,
            out_shape=jax.ShapeDtypeStruct((r, d), bf),
            in_specs=[vmem] * 3,
            out_specs=any_,
            scratch_shapes=[pltpu.VMEM((M, d), bf), dma((28,))],
            compiler_params=pltpu.CompilerParams(vmem_limit_bytes=12 * 2**20),
        )(gv, uv, acc)

    return jax.shard_map(body, mesh=mesh, in_specs=(P(("dp", "tp"), None), P("dp", "tp"), P("dp", "tp"), P("tp", "dp")), out_specs=P(("dp", "tp"), None), check_vma=False)
```

```python
import jax
import jax.numpy as jnp
from jax import lax
from jax.experimental import pallas as pl
from jax.experimental.pallas import tpu as pltpu
from jax.sharding import PartitionSpec as P

MESH = pl.DeviceIdType.MESH
M = 1024
FT = 256
NF = 14
C = 256
WC = 384
NC = 1280
MS = 512
R = 32
L0 = 6
TURN_ROW = 2688
PIECES = ((1536, 256), (1792, 256), (2048, 256), (2304, 256), (2560, 128), (2688, 128), (2816, 256), (3072, 256), (3328, 128))

O1, O2, N1, N2 = range(4)
MINE, YS, LATE = range(3)
ORDER = (
    "O1M0014Bzs", "O2M0014Bzs", "N1M0014Bz-", "N1Y0005Bk-", "O1Y0005Fk-", "O2Y0005Fk-", "N1Y0501Bkr",
    "N2M0014Bz-", "N2Y0007Bk-", "N1Y0602Fk-", "O1Y0503Fk-", "O2Y0503Fk-", "N2Y0702Bkr", "O1Y0008Sls",
    "O2Y0008Sls", "N1Y0802Fk-", "N2Y0901Fk-", "O1Y0802Fk-", "O2Y0802Fk-", "N1Y1001Fk-", "O1Y1001Fk-",
    "O2Y1001Fk-", "N2Y1001Fk-", "O1Y0803Sl-", "O1L0602Sks", "N1Y1101Fk-", "O1Y1101Fk-", "O2Y1101Fk-",
    "N2Y1101Fk-", "O2Y0804Slh", "N1Y1201Fk-", "N2Y1201Fk-", "O1Y1201Fk-", "O2Y1201Fk-", "O1Y1102Sl-",
    "N2Y1301Fk-", "N1Y1301Fk-", "O1Y1301Fk-", "O2Y1301Fk-", "O1Y1301Sk-", "O1L0802Sk-", "O1L1002Skv",
    "O2Y1202Sh-", "O2L0903Sk-", "O2L1201Sk-", "O2L1301Sk-", "O1-0001Nk-", "O1L1202Sv-",
)
JOBS = tuple((("O1", "O2", "N1", "N2").index(o[:2]), "MYL-".index(o[2]), int(o[3:5]), int(o[5:7]), int(o[7] in "BF"), int(o[7] in "BS"), o[8:])
             for o in ORDER)
NJ = len(JOBS)
AHEAD = {2: (0, 1), 3: (2, 3), 8: (6,)}
FORWARD = {9: (0, 1), 15: (2, 3), 19: (4,)}
SENDS = {9: ((0, 6), (0, 7)), 15: ((0, 8), (0, 9)), 16: ((1, 9),), 19: ((0, 10),), 25: ((0, 11),), 28: ((1, 10), (1, 11)),
         31: ((1, 12),), 35: ((1, 13),), 36: ((0, 12), (0, 13))}
TURN = 8
SPREAD = {17: (0, 1), 35: (2, 3), 40: (4, 5, 6), 43: (7,), 44: (8,)}
FINAL = (23, 29)
FETCH = 39
LEAVE = 45
SECOND = 12


def plan():
    slots, new, ahead, fresh = [], [], [], []
    group, last, seen, firsts = -1, None, 0, []
    for j, (rows, src, f0, n, s1, s2, _) in enumerate(JOBS):
        starts = bool(s1 and rows != last)
        if starts:
            group, last = group + 1, rows
            firsts.append(j)
        slots.append(max(group, 0) % 2)
        new.append(int(starts))
        top = f0 + n
        fresh.append(max(seen, f0) if src == YS and s1 and top > seen else NF)
        if src == YS and s1:
            seen = max(seen, top)
    late = 2
    load = [-1] * NJ
    for a, b in zip(firsts, firsts[1:]):
        load[b if b == late else a] = JOBS[b][0]
    return slots, new, load, fresh


SLOT, NEW, LOAD, FRESH = plan()
FIELDS = (("rows", 4), ("src", 4), ("f0", 16), ("n", 16), ("first", 2), ("second", 2), ("slot", 2), ("new", 2), ("load", 8),
          ("fresh", 16), ("before", 8), ("after", 8))


def packed(j):
    rows, src, f0, n, first, second, (before, after) = JOBS[j]
    values = (rows, src, f0, n, first, second, SLOT[j], NEW[j], LOAD[j] + 1, FRESH[j], "kzlhv".index(before), "-srhv".index(after))
    word, scale = 0, 1
    for value, (_, size) in zip(values, FIELDS):
        word, scale = word + value * scale, scale * size
    return word


def unpack(word):
    got = {}
    for name, size in FIELDS:
        got[name], word = lax.rem(word, size), lax.div(word, size)
    return got


def spot(b, gv, uv):
    per = gv.shape[1] // M
    return (gv, uv)[b // (2 * per)], b // per % 2, b % per * M


def kernel(x, wg, wu, wd, gv, uv, acc, gn, pg, pu, pd, yg, yu, yd, ld, xd, ho, hs, hr, sv, sh, prod, part,
           xv, dv, hv,
           y_send, y_recv, d_send, d_recv, w_send, w_recv, l_send, l_recv, e_send, e_recv, n_send, n_recv,
           r_send, r_recv, h_send, h_recv, t_sem, w_load, x_load, s_sem, h_sem, o_sem):
    tp, dp = lax.axis_index("tp"), lax.axis_index("dp")
    to_x = {"tp": tp + 1 - 2 * (tp % 2)}
    to_y = {"tp": tp + 2 - 4 * (tp // 2)}
    to_core = {"dp": 1 - dp}
    kd, ff = wg.shape
    dc = wd.shape[1]
    f32, bf16 = jnp.float32, jnp.bfloat16
    last = (NF - 1) * FT
    own_rows = x.shape[0]

    barrier = pltpu.get_barrier_semaphore()
    for who in (to_x, to_y, to_core):
        pl.semaphore_signal(barrier, inc=1, device_id=who, device_id_type=MESH)
    pl.semaphore_wait(barrier, 3)

    def remote(src, dst, send, recv, who):
        return pltpu.make_async_remote_copy(
            src_ref=src, dst_ref=dst, send_sem=send, recv_sem=recv, device_id=who, device_id_type=MESH)

    def pick(values, j):
        got = jnp.int32(values[0])
        for k, v in enumerate(values):
            if v != values[0]:
                got = jnp.where(j == k, v, got)
        return got

    def once(cond):
        return lambda fn: lax.fori_loop(0, jnp.where(cond, 1, 0), lambda _, c: (fn(), c)[1], 0)

    def col(t):
        return t * FT if isinstance(t, int) else pl.multiple_of(t * FT, FT)

    def tokens(q):
        return remote(x.at[pl.ds(q * C, C)], gn.at[q // (M // C), pl.ds(q % (M // C) * C, C)], n_send.at[q], n_recv.at[q], to_x)

    def mine(k, c):
        at = c * WC if isinstance(c, int) else pl.multiple_of(c * WC, WC)
        ref, peer = ((wg, pg), (wu, pu), (wd, pd))[k]
        ix = (pl.ds(at, WC),) if k == 2 else (slice(None), pl.ds(at, WC))
        return remote(ref.at[ix], peer.at[ix], w_send.at[k, c], w_recv.at[k, c], to_core)

    def y_tile(k, t, width):
        ref, mirror = ((wg, yg), (wu, yu), (wd, yd))[k]
        span = pl.ds(col(t), width)
        return ref.at[(span,) if k == 2 else (slice(None), span)], mirror.at[(0, span) if k == 2 else (0, slice(None), span)], mirror.at[(1, span) if k == 2 else (1, slice(None), span)]

    def along_y(k, t, width=FT):
        src, dst, _ = y_tile(k, t, width)
        return remote(src, dst, y_send.at[k, t], y_recv.at[k, t], to_y)

    def across(k, t, width=FT):
        _, src, dst = y_tile(k, t, width)
        return remote(src, dst, d_send.at[k, t], d_recv.at[k, t], to_core)

    def width_of(t):
        return ff - last if t == NF - 1 else FT

    def late_send(p):
        row, n = PIECES[p]
        dst = ld.at[0, pl.ds(row - L0 * FT, n)]
        if row < TURN_ROW:
            return remote(yd.at[0, pl.ds(row, n)], dst, l_send.at[p], l_recv.at[p], to_x)
        return remote(xd.at[pl.ds(row - TURN_ROW, n)], dst, l_send.at[p], l_recv.at[p], to_y)

    def late_across(p):
        row, n = PIECES[p]
        at = pl.ds(row - L0 * FT, n)
        return remote(ld.at[0, at], ld.at[1, at], e_send.at[p], e_recv.at[p], to_core)

    def turn():
        return remote(wd.at[pl.ds(TURN_ROW, ff - TURN_ROW)], xd, t_sem.at[0], t_sem.at[1], to_x)

    def hidden(k, t, end=False):
        at = (k, t, slice(None), pl.ds(NF * FT - ff, ff - last)) if end else (k, t)
        return remote(hs.at[at], hr.at[at], h_send.at[k, t], h_recv.at[k, t], to_x)

    def products(k, q):
        rows = pl.ds(q * C, C)
        return remote(prod.at[k, rows], part.at[k, rows], r_send.at[k, q], r_recv.at[k, q], to_x)

    for q in range(own_rows // C):
        tokens(q).start()
    turn().start()
    for t in range(NF):
        for k in range(3):
            along_y(k, t, width_of(t)).start()
    for c in range(ff // WC):
        for k in range(3):
            mine(k, c).start()

    def tile_at(f):
        return pl.multiple_of(lax.min(f * FT, ff - FT), 128)

    def halves(extent):
        return [pl.ds(pl.multiple_of(core * extent, 128), extent) for core in (dp, 1 - dp)]

    def load_first(slot, f, src):
        at = tile_at(f)
        copies = []
        for k, (pair, dst) in enumerate((((wg, pg) if src == MINE else (yg.at[0], yg.at[1]), gv),
                                         ((wu, pu) if src == MINE else (yu.at[0], yu.at[1]), uv))):
            for m, (ref, rows) in enumerate(zip(pair, halves(kd))):
                copies.append(pltpu.make_async_copy(ref.at[:, pl.ds(at, FT)], dst.at[slot, rows], w_load.at[slot, 2 * k + m]))
        return copies

    def load_second(slot, f, src):
        at = tile_at(f) if src != LATE else pl.multiple_of(tile_at(f) - L0 * FT, 128)
        pair = {MINE: (wd, pd), YS: (yd.at[0], yd.at[1]), LATE: (ld.at[0], ld.at[1])}[src]
        return [pltpu.make_async_copy(ref.at[pl.ds(at, FT)], dv.at[slot, :, cols], w_load.at[slot, 4 + m])
                for m, (ref, cols) in enumerate(zip(pair, halves(dc)))]

    def load_h(slot, rows, f, src, end=False):
        cols = pl.ds(NF * FT - ff, ff - last) if end else slice(None)
        return pltpu.make_async_copy((hr if src == LATE else ho).at[rows, f, :, cols], hv.at[slot, :, cols], w_load.at[slot, 6])

    def load_x(rows, slot):
        own = pltpu.make_async_copy(x.at[pl.ds(pl.multiple_of(lax.min(rows, 1) * M, M), M)], xv.at[slot], x_load.at[slot])
        other = pltpu.make_async_copy(gn.at[lax.max(rows - 2, 0)], xv.at[slot], x_load.at[slot])
        return own, other

    def start_x(rows, slot):
        @pl.when(rows < N1)
        def _():
            load_x(rows, slot)[0].start()

        @pl.when(rows >= N1)
        def _():
            load_x(rows, slot)[1].start()

    def send_across(t, wait_first=True):
        for k in range(3):
            along_y(k, t, width_of(t)).wait_recv()
        for k in range(3):
            across(k, t, width_of(t)).start()

    def prefetch(slot, rows, src, f, first, second, fresh):
        def start(*groups):
            for copies in groups:
                for copy in copies:
                    copy.start()

        @once(src == MINE)
        def _():
            @pl.when((rows == O1) & (f % 3 != 2) & (f < NF - 1))
            def _():
                for k in range(3):
                    mine(k, (2 * f + 2) // 3).wait_recv()
            start(load_first(slot, f, MINE), load_second(slot, f, MINE))

        @once(src == YS)
        def _():
            @once((first == 1) & (f >= fresh))
            def _():
                early = [t for ts in AHEAD.values() for t in ts]
                to_send = f < NF - 1
                for t in early:
                    to_send = to_send & (f != t)

                @pl.when(to_send)
                def _():
                    for k in range(3):
                        along_y(k, f).wait_recv()
                    for k in range(3):
                        across(k, f).start()

                @pl.when(f < NF - 1)
                def _():
                    for k in range(3):
                        across(k, f).wait_recv()

                @pl.when(f == NF - 1)
                def _():
                    send_across(NF - 1)
                    for k in range(3):
                        across(k, NF - 1, width_of(NF - 1)).wait_recv()

            @pl.when(first == 1)
            def _():
                start(load_first(slot, f, YS))

            @pl.when(first == 0)
            def _():
                load_h(slot, rows, f, YS).start()

            @pl.when(second == 1)
            def _():
                start(load_second(slot, f, YS))

        @once(src == LATE)
        def _():
            @pl.when(f < NF - 1)
            def _():
                hidden(rows, f).wait_recv()
                load_h(slot, rows, f, LATE).start()

            @pl.when(f == NF - 1)
            def _():
                hidden(rows, NF - 1, True).wait_recv()
                hv[slot, :, pl.ds(0, NF * FT - ff)] = jnp.zeros((M, NF * FT - ff), bf16)
                load_h(slot, rows, NF - 1, LATE, True).start()
            for t in range(L0, NF):
                @pl.when((rows == (O1 if t < SECOND else O2)) & (f == t))
                def _():
                    for p, (row, _) in enumerate(PIECES):
                        if row // FT == t:
                            late_across(p).wait_recv()
            start(load_second(slot, f, LATE))

    def store_h(slot, rows, f):
        return (pltpu.make_async_copy(hv.at[slot], ho.at[lax.min(rows, 1), f], h_sem.at[slot]),
                pltpu.make_async_copy(hv.at[slot], hs.at[lax.max(rows - 2, 0), f], h_sem.at[slot]))

    def swap(k, out):
        return pltpu.make_async_copy(acc, sv.at[k], s_sem) if out else pltpu.make_async_copy(sv.at[k], acc, s_sem)

    def store(k, q, slot):
        rows = pl.ds(q * C, C)
        return pltpu.make_async_copy(xv.at[slot, rows], prod.at[k, rows], o_sem.at[q])

    start_x(jnp.int32(O1), 0)
    prefetch(0, jnp.int32(O1), jnp.int32(MINE), jnp.int32(0), jnp.int32(1), jnp.int32(1), jnp.int32(NF))

    words = [packed(j) for j in range(NJ)]

    def job(j, carry):
        step0, word, own_h_before = carry
        this = unpack(word)
        rows, src, f0, n, first, second = (this[k] for k in ("rows", "src", "f0", "n", "first", "second"))
        word_n = pick(words[1:] + words[-1:], j)
        nxt = unpack(word_n)
        fresh, slot_x, load_n = this["fresh"], this["slot"], this["load"] - 1
        is_h = (first == 1) & (second == 0)

        def is_mode(at, what):
            return this["after" if at else "before"] == ("-srhv" if at else "kzlhv").index(what)

        for at, tiles in AHEAD.items():
            @once(j == at)
            def _():
                for t in tiles:
                    send_across(t)
        @once(j == 2)
        def _():
            for q in range(M // C):
                tokens(q).wait_recv()
        @once(j == 6)
        def _():
            for q in range(M // C, own_rows // C):
                tokens(q).wait_recv()
        @once(j == TURN)
        def _():
            turn().wait_recv()
            for p, (row, _) in enumerate(PIECES):
                if row >= TURN_ROW:
                    late_send(p).start()
        for at, ps in SPREAD.items():
            @once(j == at)
            def _():
                for p in ps:
                    late_send(p).wait_recv()
                for p in ps:
                    late_across(p).start()

        new = this["new"] == 1
        @once(j == 2)
        def _():
            start_x(rows, slot_x)

        @pl.when(new)
        def _():
            load_x(rows, slot_x)[0].wait()

        @pl.when((load_n >= 0) & (j != 2))
        def _():
            start_x(load_n, 1 - slot_x)

        @once(j == 2)
        def _():
            start_x(jnp.int32(JOBS[4][0]), 1 - slot_x)

        @once(is_mode(0, "z"))
        def _():
            @pl.loop(0, M // R)
            def _(r):
                acc[pl.ds(pl.multiple_of(r * R, R), R)] = jnp.zeros((R, acc.shape[1]), f32)

        @once(is_mode(0, "l"))
        def _():
            swap(rows, False).start()
            swap(rows, False).wait()

        def to_rows(slot):
            @pl.loop(0, M // R)
            def _(r):
                at = pl.ds(pl.multiple_of(r * R, R), R)
                xv[slot, at] = acc[at].astype(bf16)

        def from_rows(slot):
            @pl.loop(0, M // R)
            def _(r):
                at = pl.ds(pl.multiple_of(r * R, R), R)
                acc[at] = xv[slot, at].astype(f32)

        @once(j == FETCH)
        def _():
            pltpu.make_async_copy(sh, xv.at[1], x_load.at[1]).start()

        @once(is_mode(0, "h"))
        def _():
            pltpu.make_async_copy(sh, xv.at[1], x_load.at[1]).wait()
            from_rows(1)

        @once(is_mode(0, "v"))
        def _():
            from_rows(0)

        for k, at_job in enumerate(FINAL):
            @once(j == at_job)
            def _():
                for q in range(M // C):
                    products(k, q).wait_recv()
                for ref in (x.at[pl.ds(k * M, M)], part.at[k]):
                    copy = pltpu.make_async_copy(ref, xv.at[slot_x], x_load.at[slot_x])
                    copy.start()
                    copy.wait()

                    @pl.loop(0, M // R)
                    def _(r):
                        at = pl.ds(pl.multiple_of(r * R, R), R)
                        acc[at] = acc[at] + xv[slot_x, at].astype(f32)

        def step(i, _):
            f = f0 + i
            slot = (step0 + i) % 2
            ends = i + 1 == n

            @pl.when(jnp.where(i == 0, own_h_before == 1, is_h))
            def _():
                store_h(1 - slot, rows, f)[0].wait()

            @pl.when(first == 1)
            def _():
                for copy in load_first(slot, f, MINE):
                    copy.wait()

            @pl.when(second == 1)
            def _():
                for copy in load_second(slot, f, MINE):
                    copy.wait()

            half_h = (src == LATE) & (f == NF - 1)

            @pl.when((first == 0) & (second == 1) & jnp.logical_not(half_h))
            def _():
                load_h(slot, rows, f, YS).wait()

            @pl.when(half_h)
            def _():
                load_h(slot, rows, f, YS, True).wait()

            @pl.when(jnp.logical_not(ends & (j == NJ - 1)))
            def _():
                prefetch(1 - slot, *[jnp.where(ends, nxt[k], f + 1 if k == "f0" else this[k])
                                     for k in ("rows", "src", "f0", "first", "second", "fresh")])

            @pl.when(first == 1)
            def _():
                skip = lax.max(f * FT - (ff - FT), 0)
                own = lax.broadcasted_iota(jnp.int32, (MS, FT), 1) >= skip
                for r in range(0, M, MS):
                    at = slice(r, r + MS)
                    a = jnp.dot(xv[slot_x, at], gv[slot], preferred_element_type=f32)
                    b = jnp.dot(xv[slot_x, at], uv[slot], preferred_element_type=f32)
                    hv[slot, at] = jnp.where(own, a * jax.nn.sigmoid(a) * b, 0.0).astype(bf16)

            @pl.when(second == 1)
            def _():
                for c in range(0, acc.shape[1], NC):
                    cols = slice(c, c + NC)
                    acc[:, cols] += jnp.dot(hv[slot], dv[slot, :, cols], preferred_element_type=f32)

            @pl.when(is_h & (rows < N1))
            def _():
                store_h(slot, rows, f)[0].start()

            @pl.when(is_h & (rows >= N1))
            def _():
                store_h(slot, rows, f)[1].start()
            return 0

        lax.fori_loop(0, n, step, 0)

        @pl.when(is_h & (rows >= N1))
        def _():
            store_h((step0 + n - 1) % 2, rows, f0)[1].wait()

        for at, pairs in SENDS.items():
            @once(j == at)
            def _():
                for k, t in pairs:
                    hidden(k, t, t == NF - 1).start()

        for at, ps in FORWARD.items():
            @once(j == at)
            def _():
                for p in ps:
                    late_send(p).start()

        @once(is_mode(1, "s"))
        def _():
            swap(rows, True).start()
            swap(rows, True).wait()

        @once(is_mode(1, "h"))
        def _():
            to_rows(slot_x)
            copy = pltpu.make_async_copy(xv.at[slot_x], sh, s_sem)
            copy.start()
            copy.wait()

        @once(is_mode(1, "v"))
        def _():
            to_rows(0)

        @once(is_mode(1, "r"))
        def _():
            for q in range(M // C):
                @pl.loop(0, C // R)
                def _(r):
                    at = pl.ds(pl.multiple_of(q * C + r * R, R), R)
                    xv[slot_x, at] = acc[at].astype(bf16)
                store(rows - 2, q, slot_x).start()
            for q in range(M // C):
                store(rows - 2, q, slot_x).wait()
                products(rows - 2, q).start()

        @once(j == LEAVE)
        def _():
            @pl.loop(0, M // R)
            def _(r):
                for b in range(acc.shape[1] // FT):
                    buf, k, row = spot(b, gv, uv)
                    at = pl.ds(pl.multiple_of(r * R, R), R)
                    buf[k, pl.ds(pl.multiple_of(row + r * R, R), R)] = acc[at, b * FT:(b + 1) * FT].astype(bf16)
        return step0 + n, word_n, (is_h & (rows < N1)).astype(jnp.int32)

    lax.fori_loop(0, NJ, job, (jnp.int32(0), jnp.int32(words[0]), jnp.int32(0)))

    for q in range(own_rows // C):
        tokens(q).wait_send()
    turn().wait_send()
    for t in range(NF):
        for k in range(3):
            along_y(k, t, width_of(t)).wait_send()
            across(k, t, width_of(t)).wait_send()
    for c in range(ff // WC):
        for k in range(3):
            mine(k, c).wait_send()
    for p in range(len(PIECES)):
        late_send(p).wait_send()
        late_across(p).wait_send()
    for k in range(2):
        for q in range(M // C):
            products(k, q).wait_send()
    for pairs in SENDS.values():
        for k, t in pairs:
            hidden(k, t, t == NF - 1).wait_send()


def write(gv, uv, acc, out, yv, sem):
    step = 128
    early, late = [], []
    for b in range(out.shape[1] // FT):
        buf, k, row = spot(b, gv, uv)
        early.append(pltpu.make_async_copy(buf.at[k, pl.ds(row, M)], out.at[pl.ds(M, M), pl.ds(b * FT, FT)], sem.at[b]))
    for k in range(M // step):
        late.append(pltpu.make_async_copy(yv.at[pl.ds(k * step, step)], out.at[pl.ds(k * step, step)], sem.at[len(early) + k]))
    for copy in early:
        copy.start()
    for k, copy in enumerate(late):
        @pl.loop(0, step // R)
        def _(r):
            at = pl.ds(pl.multiple_of(k * step + r * R, R), R)
            yv[at] = acc[at].astype(jnp.bfloat16)
        copy.start()
    for copy in early + late:
        copy.wait()


def solution(mesh):
    def body(x, wg, wu, wd):
        r, d = x.shape
        kd, ff = wg.shape
        dc = wd.shape[1]
        bf, f32 = jnp.bfloat16, jnp.float32
        any_ = pl.BlockSpec(memory_space=pl.ANY)
        vmem = pl.BlockSpec(memory_space=pltpu.VMEM)
        nh = (2, NF, M, FT)
        shapes = [(2, M, d), (kd, ff), (kd, ff), (ff, dc), (2, kd, ff), (2, kd, ff), (2, ff, dc),
                  (2, ff - L0 * FT, dc), (ff - TURN_ROW, dc), nh, nh, nh]
        dma = pltpu.SemaphoreType.DMA
        nl, nn, nw = len(PIECES), r // C, ff // WC
        work = [jax.ShapeDtypeStruct(s, bf) for s in shapes] + [
            jax.ShapeDtypeStruct((2, M, d), f32), jax.ShapeDtypeStruct((M, d), bf), jax.ShapeDtypeStruct((2, M, d), bf), jax.ShapeDtypeStruct((2, M, d), bf)]
        gv, uv, acc, *_ = pl.pallas_call(
            kernel,
            out_shape=[pltpu.VMEM((2, d, FT), bf)] * 2 + [pltpu.VMEM((M, d), f32)] + work,
            in_specs=[any_] * 4,
            out_specs=[vmem] * 3 + [any_] * len(work),
            scratch_shapes=[
                pltpu.VMEM((2, M, d), bf), pltpu.VMEM((2, FT, d), bf), pltpu.VMEM((2, M, FT), bf),
                dma((3, NF)), dma((3, NF)), dma((3, NF)), dma((3, NF)), dma((3, nw)), dma((3, nw)),
                dma((nl,)), dma((nl,)), dma((nl,)), dma((nl,)), dma((nn,)), dma((nn,)),
                dma((2, M // C)), dma((2, M // C)), dma((2, NF)), dma((2, NF)), dma((2,)),
                dma((2, 7)), dma((2,)), dma, dma((2,)), dma((M // C,)),
            ],
            compiler_params=pltpu.CompilerParams(collective_id=0, has_side_effects=True, vmem_limit_bytes=int(33.9 * 2**20)),
        )(x, wg, wu, wd)
        return pl.pallas_call(
            write,
            out_shape=jax.ShapeDtypeStruct((r, d), bf),
            in_specs=[vmem] * 3,
            out_specs=any_,
            scratch_shapes=[pltpu.VMEM((M, d), bf), dma((28,))],
            compiler_params=pltpu.CompilerParams(vmem_limit_bytes=12 * 2**20),
        )(gv, uv, acc)

    return jax.shard_map(body, mesh=mesh, in_specs=(P(("dp", "tp"), None), P("dp", "tp"), P("dp", "tp"), P("tp", "dp")), out_specs=P(("dp", "tp"), None), check_vma=False)
```

```python
import jax
import jax.numpy as jnp
from jax import lax
from jax.experimental import pallas as pl
from jax.experimental.pallas import tpu as pltpu
from jax.sharding import PartitionSpec as P

MESH = pl.DeviceIdType.MESH
M = 1024
FT = 256
NF = 14
C = 256
WC = 384
NC = 1280
MS = 512
R = 32
L0 = 6
TURN_ROW = 2688
PIECES = ((1536, 256), (1792, 256), (2048, 256), (2304, 256), (2560, 128), (2688, 128), (2816, 256), (3072, 256), (3328, 128))

O1, O2, N1, N2 = range(4)
MINE, YS, LATE = range(3)
ORDER = (
    "O1M0014Bzs", "O2M0014Bzs", "N1M0014Bz-", "N1Y0005Bk-", "O1Y0005Fk-", "O2Y0005Fk-", "N1Y0501Bkr",
    "N2M0014Bz-", "N2Y0007Bk-", "N1Y0602Fk-", "O1Y0503Fk-", "O2Y0503Fk-", "N2Y0702Bkr", "O1Y0008Sls",
    "O2Y0008Sls", "N1Y0802Fk-", "N2Y0901Fk-", "O1Y0802Fk-", "O2Y0802Fk-", "N1Y1001Fk-", "O1Y1001Fk-",
    "O2Y1001Fk-", "N2Y1001Fk-", "O1Y0803Sl-", "O1L0602Sks", "N1Y1101Fk-", "O1Y1101Fk-", "O2Y1101Fk-",
    "N2Y1101Fk-", "O2Y0804Slh", "N1Y1201Fk-", "N2Y1201Fk-", "O1Y1201Fk-", "O2Y1201Fk-", "O1Y1102Sl-",
    "N2Y1301Fk-", "N1Y1301Fk-", "O1Y1301Fk-", "O2Y1301Fk-", "O1Y1301Sk-", "O1L0802Sk-", "O1L1002Skv",
    "O2Y1202Sh-", "O2L0903Sk-", "O2L1201Sk-", "O2L1301Sk-", "O1-0001Nk-", "O1L1202Sv-",
)
JOBS = tuple((("O1", "O2", "N1", "N2").index(o[:2]), "MYL-".index(o[2]), int(o[3:5]), int(o[5:7]), int(o[7] in "BF"), int(o[7] in "BS"), o[8:])
             for o in ORDER)
NJ = len(JOBS)
AHEAD = {2: (0, 1), 3: (2, 3), 8: (6,)}
FORWARD = {9: (0, 1), 15: (2, 3), 19: (4,)}
SENDS = {9: ((0, 6), (0, 7)), 15: ((0, 8), (0, 9)), 16: ((1, 9),), 19: ((0, 10),), 25: ((0, 11),), 28: ((1, 10), (1, 11)),
         31: ((1, 12),), 35: ((1, 13),), 36: ((0, 12), (0, 13))}
TURN = 8
SPREAD = {17: (0, 1), 35: (2, 3), 40: (4, 5, 6), 43: (7,), 44: (8,)}
FINAL = (23, 29)
FETCH = 39
LEAVE = 45
SECOND = 12


def plan():
    slots, new, ahead, fresh = [], [], [], []
    group, last, seen, firsts = -1, None, 0, []
    for j, (rows, src, f0, n, s1, s2, _) in enumerate(JOBS):
        starts = bool(s1 and rows != last)
        if starts:
            group, last = group + 1, rows
            firsts.append(j)
        slots.append(max(group, 0) % 2)
        new.append(int(starts))
        top = f0 + n
        fresh.append(max(seen, f0) if src == YS and s1 and top > seen else NF)
        if src == YS and s1:
            seen = max(seen, top)
    late = 2
    load = [-1] * NJ
    for a, b in zip(firsts, firsts[1:]):
        load[b if b == late else a] = JOBS[b][0]
    return slots, new, load, fresh


SLOT, NEW, LOAD, FRESH = plan()
FIELDS = (("rows", 4), ("src", 4), ("f0", 16), ("n", 16), ("first", 2), ("second", 2), ("slot", 2), ("new", 2), ("load", 8),
          ("fresh", 16), ("before", 8), ("after", 8))


def packed(j):
    rows, src, f0, n, first, second, (before, after) = JOBS[j]
    values = (rows, src, f0, n, first, second, SLOT[j], NEW[j], LOAD[j] + 1, FRESH[j], "kzlhv".index(before), "-srhv".index(after))
    word, scale = 0, 1
    for value, (_, size) in zip(values, FIELDS):
        word, scale = word + value * scale, scale * size
    return word


def unpack(word):
    got = {}
    for name, size in FIELDS:
        got[name], word = lax.rem(word, size), lax.div(word, size)
    return got


def spot(b, gv, uv):
    per = gv.shape[1] // M
    return (gv, uv)[b // (2 * per)], b // per % 2, b % per * M


def kernel(x, wg, wu, wd, gv, uv, acc, gn, pg, pu, pd, yg, yu, yd, ld, xd, ho, hs, hr, sv, sh, prod, part,
           xv, dv, hv,
           y_send, y_recv, d_send, d_recv, w_send, w_recv, l_send, l_recv, e_send, e_recv, n_send, n_recv,
           r_send, r_recv, h_send, h_recv, t_sem, w_load, x_load, s_sem, h_sem, o_sem):
    tp, dp = lax.axis_index("tp"), lax.axis_index("dp")
    to_x = {"tp": tp + 1 - 2 * (tp % 2)}
    to_y = {"tp": tp + 2 - 4 * (tp // 2)}
    to_core = {"dp": 1 - dp}
    kd, ff = wg.shape
    dc = wd.shape[1]
    f32, bf16 = jnp.float32, jnp.bfloat16
    last = (NF - 1) * FT
    own_rows = x.shape[0]

    barrier = pltpu.get_barrier_semaphore()
    for who in (to_x, to_y, to_core):
        pl.semaphore_signal(barrier, inc=1, device_id=who, device_id_type=MESH)
    pl.semaphore_wait(barrier, 3)

    def remote(src, dst, send, recv, who):
        return pltpu.make_async_remote_copy(
            src_ref=src, dst_ref=dst, send_sem=send, recv_sem=recv, device_id=who, device_id_type=MESH)

    def pick(values, j):
        got = jnp.int32(values[0])
        for k, v in enumerate(values):
            if v != values[0]:
                got = jnp.where(j == k, v, got)
        return got

    def col(t):
        return t * FT if isinstance(t, int) else pl.multiple_of(t * FT, FT)

    def tokens(q):
        return remote(x.at[pl.ds(q * C, C)], gn.at[q // (M // C), pl.ds(q % (M // C) * C, C)], n_send.at[q], n_recv.at[q], to_x)

    def mine(k, c):
        at = c * WC if isinstance(c, int) else pl.multiple_of(c * WC, WC)
        ref, peer = ((wg, pg), (wu, pu), (wd, pd))[k]
        ix = (pl.ds(at, WC),) if k == 2 else (slice(None), pl.ds(at, WC))
        return remote(ref.at[ix], peer.at[ix], w_send.at[k, c], w_recv.at[k, c], to_core)

    def y_tile(k, t, width):
        ref, mirror = ((wg, yg), (wu, yu), (wd, yd))[k]
        span = pl.ds(col(t), width)
        return ref.at[(span,) if k == 2 else (slice(None), span)], mirror.at[(0, span) if k == 2 else (0, slice(None), span)], mirror.at[(1, span) if k == 2 else (1, slice(None), span)]

    def along_y(k, t, width=FT):
        src, dst, _ = y_tile(k, t, width)
        return remote(src, dst, y_send.at[k, t], y_recv.at[k, t], to_y)

    def across(k, t, width=FT):
        _, src, dst = y_tile(k, t, width)
        return remote(src, dst, d_send.at[k, t], d_recv.at[k, t], to_core)

    def width_of(t):
        return ff - last if t == NF - 1 else FT

    def late_send(p):
        row, n = PIECES[p]
        dst = ld.at[0, pl.ds(row - L0 * FT, n)]
        if row < TURN_ROW:
            return remote(yd.at[0, pl.ds(row, n)], dst, l_send.at[p], l_recv.at[p], to_x)
        return remote(xd.at[pl.ds(row - TURN_ROW, n)], dst, l_send.at[p], l_recv.at[p], to_y)

    def late_across(p):
        row, n = PIECES[p]
        at = pl.ds(row - L0 * FT, n)
        return remote(ld.at[0, at], ld.at[1, at], e_send.at[p], e_recv.at[p], to_core)

    def turn():
        return remote(wd.at[pl.ds(TURN_ROW, ff - TURN_ROW)], xd, t_sem.at[0], t_sem.at[1], to_x)

    def hidden(k, t, end=False):
        at = (k, t, slice(None), pl.ds(NF * FT - ff, ff - last)) if end else (k, t)
        return remote(hs.at[at], hr.at[at], h_send.at[k, t], h_recv.at[k, t], to_x)

    def products(k, q):
        rows = pl.ds(q * C, C)
        return remote(prod.at[k, rows], part.at[k, rows], r_send.at[k, q], r_recv.at[k, q], to_x)

    for q in range(own_rows // C):
        tokens(q).start()
    turn().start()
    for t in range(NF):
        for k in range(3):
            along_y(k, t, width_of(t)).start()
    for c in range(ff // WC):
        for k in range(3):
            mine(k, c).start()

    def tile_at(f):
        return pl.multiple_of(lax.min(f * FT, ff - FT), 128)

    def halves(extent):
        return [pl.ds(pl.multiple_of(core * extent, 128), extent) for core in (dp, 1 - dp)]

    def load_first(slot, f, src):
        at = tile_at(f)
        copies = []
        for k, (pair, dst) in enumerate((((wg, pg) if src == MINE else (yg.at[0], yg.at[1]), gv),
                                         ((wu, pu) if src == MINE else (yu.at[0], yu.at[1]), uv))):
            for m, (ref, rows) in enumerate(zip(pair, halves(kd))):
                copies.append(pltpu.make_async_copy(ref.at[:, pl.ds(at, FT)], dst.at[slot, rows], w_load.at[slot, 2 * k + m]))
        return copies

    def load_second(slot, f, src):
        at = tile_at(f) if src != LATE else pl.multiple_of(tile_at(f) - L0 * FT, 128)
        pair = {MINE: (wd, pd), YS: (yd.at[0], yd.at[1]), LATE: (ld.at[0], ld.at[1])}[src]
        return [pltpu.make_async_copy(ref.at[pl.ds(at, FT)], dv.at[slot, :, cols], w_load.at[slot, 4 + m])
                for m, (ref, cols) in enumerate(zip(pair, halves(dc)))]

    def load_h(slot, rows, f, src, end=False):
        cols = pl.ds(NF * FT - ff, ff - last) if end else slice(None)
        return pltpu.make_async_copy((hr if src == LATE else ho).at[rows, f, :, cols], hv.at[slot, :, cols], w_load.at[slot, 6])

    def load_x(rows, slot):
        own = pltpu.make_async_copy(x.at[pl.ds(pl.multiple_of(lax.min(rows, 1) * M, M), M)], xv.at[slot], x_load.at[slot])
        other = pltpu.make_async_copy(gn.at[lax.max(rows - 2, 0)], xv.at[slot], x_load.at[slot])
        return own, other

    def start_x(rows, slot):
        @pl.when(rows < N1)
        def _():
            load_x(rows, slot)[0].start()

        @pl.when(rows >= N1)
        def _():
            load_x(rows, slot)[1].start()

    def send_across(t, wait_first=True):
        for k in range(3):
            along_y(k, t, width_of(t)).wait_recv()
        for k in range(3):
            across(k, t, width_of(t)).start()

    def prefetch(slot, rows, src, f, first, second, fresh):
        @pl.when((src == MINE) & (rows == O1) & (f % 3 != 2) & (f < NF - 1))
        def _():
            for k in range(3):
                mine(k, (2 * f + 2) // 3).wait_recv()

        is_new = (src == YS) & (first == 1) & (f >= fresh)
        early = [t for ts in AHEAD.values() for t in ts]
        to_send = is_new
        for t in early:
            to_send = to_send & (f != t)

        @pl.when(to_send & (f < NF - 1))
        def _():
            for k in range(3):
                along_y(k, f).wait_recv()
            for k in range(3):
                across(k, f).start()

        @pl.when(is_new & (f < NF - 1))
        def _():
            for k in range(3):
                across(k, f).wait_recv()

        @pl.when(is_new & (f == NF - 1))
        def _():
            send_across(NF - 1)
            for k in range(3):
                across(k, NF - 1, width_of(NF - 1)).wait_recv()

        @pl.when((src == LATE) & (f < NF - 1))
        def _():
            hidden(rows, f).wait_recv()

        @pl.when((src == LATE) & (f == NF - 1))
        def _():
            hidden(rows, NF - 1, True).wait_recv()
            hv[slot, :, pl.ds(0, NF * FT - ff)] = jnp.zeros((M, NF * FT - ff), bf16)
            load_h(slot, rows, NF - 1, LATE, True).start()

        for t in range(L0, NF):
            @pl.when((src == LATE) & (rows == (O1 if t < SECOND else O2)) & (f == t))
            def _():
                for p, (row, _) in enumerate(PIECES):
                    if row // FT == t:
                        late_across(p).wait_recv()

        for value in (MINE, YS):
            @pl.when((first == 1) & (src == value))
            def _():
                for copy in load_first(slot, f, value):
                    copy.start()
        for value in (MINE, YS, LATE):
            @pl.when((second == 1) & (src == value))
            def _():
                for copy in load_second(slot, f, value):
                    copy.start()
        for value in (YS, LATE):
            @pl.when((first == 0) & (src == value) & ((src == YS) | (f < NF - 1)))
            def _():
                load_h(slot, rows, f, value).start()

    def store_h(slot, rows, f):
        return (pltpu.make_async_copy(hv.at[slot], ho.at[lax.min(rows, 1), f], h_sem.at[slot]),
                pltpu.make_async_copy(hv.at[slot], hs.at[lax.max(rows - 2, 0), f], h_sem.at[slot]))

    def swap(k, out):
        return pltpu.make_async_copy(acc, sv.at[k], s_sem) if out else pltpu.make_async_copy(sv.at[k], acc, s_sem)

    def store(k, q, slot):
        rows = pl.ds(q * C, C)
        return pltpu.make_async_copy(xv.at[slot, rows], prod.at[k, rows], o_sem.at[q])

    start_x(jnp.int32(O1), 0)
    prefetch(0, jnp.int32(O1), jnp.int32(MINE), jnp.int32(0), jnp.int32(1), jnp.int32(1), jnp.int32(NF))

    words = [packed(j) for j in range(NJ)]

    def job(j, carry):
        step0, word, own_h_before = carry
        this = unpack(word)
        rows, src, f0, n, first, second = (this[k] for k in ("rows", "src", "f0", "n", "first", "second"))
        word_n = pick(words[1:] + words[-1:], j)
        nxt = unpack(word_n)
        fresh, slot_x, load_n = this["fresh"], this["slot"], this["load"] - 1
        is_h = (first == 1) & (second == 0)

        def is_mode(at, what):
            return this["after" if at else "before"] == ("-srhv" if at else "kzlhv").index(what)

        for at, tiles in AHEAD.items():
            @pl.when(j == at)
            def _():
                for t in tiles:
                    send_across(t)
        @pl.when(j == 2)
        def _():
            for q in range(M // C):
                tokens(q).wait_recv()
        @pl.when(j == 6)
        def _():
            for q in range(M // C, own_rows // C):
                tokens(q).wait_recv()
        @pl.when(j == TURN)
        def _():
            turn().wait_recv()
            for p, (row, _) in enumerate(PIECES):
                if row >= TURN_ROW:
                    late_send(p).start()
        for at, ps in SPREAD.items():
            @pl.when(j == at)
            def _():
                for p in ps:
                    late_send(p).wait_recv()
                for p in ps:
                    late_across(p).start()

        new = this["new"] == 1
        @pl.when(j == 2)
        def _():
            start_x(rows, slot_x)

        @pl.when(new)
        def _():
            load_x(rows, slot_x)[0].wait()

        @pl.when((load_n >= 0) & (j != 2))
        def _():
            start_x(load_n, 1 - slot_x)

        @pl.when(j == 2)
        def _():
            start_x(jnp.int32(JOBS[4][0]), 1 - slot_x)

        @pl.when(is_mode(0, "z"))
        def _():
            @pl.loop(0, M // R)
            def _(r):
                acc[pl.ds(pl.multiple_of(r * R, R), R)] = jnp.zeros((R, acc.shape[1]), f32)

        @pl.when(is_mode(0, "l"))
        def _():
            swap(rows, False).start()
            swap(rows, False).wait()

        def to_rows(slot):
            @pl.loop(0, M // R)
            def _(r):
                at = pl.ds(pl.multiple_of(r * R, R), R)
                xv[slot, at] = acc[at].astype(bf16)

        def from_rows(slot):
            @pl.loop(0, M // R)
            def _(r):
                at = pl.ds(pl.multiple_of(r * R, R), R)
                acc[at] = xv[slot, at].astype(f32)

        @pl.when(j == FETCH)
        def _():
            pltpu.make_async_copy(sh, xv.at[1], x_load.at[1]).start()

        @pl.when(is_mode(0, "h"))
        def _():
            pltpu.make_async_copy(sh, xv.at[1], x_load.at[1]).wait()
            from_rows(1)

        @pl.when(is_mode(0, "v"))
        def _():
            from_rows(0)

        for k, at_job in enumerate(FINAL):
            @pl.when(j == at_job)
            def _():
                for q in range(M // C):
                    products(k, q).wait_recv()
                for ref in (x.at[pl.ds(k * M, M)], part.at[k]):
                    copy = pltpu.make_async_copy(ref, xv.at[slot_x], x_load.at[slot_x])
                    copy.start()
                    copy.wait()

                    @pl.loop(0, M // R)
                    def _(r):
                        at = pl.ds(pl.multiple_of(r * R, R), R)
                        acc[at] = acc[at] + xv[slot_x, at].astype(f32)

        def step(i, _):
            f = f0 + i
            slot = (step0 + i) % 2
            ends = i + 1 == n

            @pl.when(jnp.where(i == 0, own_h_before == 1, is_h))
            def _():
                store_h(1 - slot, rows, f)[0].wait()

            @pl.when(first == 1)
            def _():
                for copy in load_first(slot, f, MINE):
                    copy.wait()

            @pl.when(second == 1)
            def _():
                for copy in load_second(slot, f, MINE):
                    copy.wait()

            half_h = (src == LATE) & (f == NF - 1)

            @pl.when((first == 0) & (second == 1) & jnp.logical_not(half_h))
            def _():
                load_h(slot, rows, f, YS).wait()

            @pl.when(half_h)
            def _():
                load_h(slot, rows, f, YS, True).wait()

            @pl.when(jnp.logical_not(ends & (j == NJ - 1)))
            def _():
                prefetch(1 - slot, *[jnp.where(ends, nxt[k], f + 1 if k == "f0" else this[k])
                                     for k in ("rows", "src", "f0", "first", "second", "fresh")])

            @pl.when(first == 1)
            def _():
                skip = lax.max(f * FT - (ff - FT), 0)
                own = lax.broadcasted_iota(jnp.int32, (MS, FT), 1) >= skip
                for r in range(0, M, MS):
                    at = slice(r, r + MS)
                    a = jnp.dot(xv[slot_x, at], gv[slot], preferred_element_type=f32)
                    b = jnp.dot(xv[slot_x, at], uv[slot], preferred_element_type=f32)
                    hv[slot, at] = jnp.where(own, a * jax.nn.sigmoid(a) * b, 0.0).astype(bf16)

            @pl.when(second == 1)
            def _():
                for c in range(0, acc.shape[1], NC):
                    cols = slice(c, c + NC)
                    acc[:, cols] += jnp.dot(hv[slot], dv[slot, :, cols], preferred_element_type=f32)

            @pl.when(is_h & (rows < N1))
            def _():
                store_h(slot, rows, f)[0].start()

            @pl.when(is_h & (rows >= N1))
            def _():
                store_h(slot, rows, f)[1].start()
            return 0

        lax.fori_loop(0, n, step, 0)

        @pl.when(is_h & (rows >= N1))
        def _():
            store_h((step0 + n - 1) % 2, rows, f0)[1].wait()

        for at, pairs in SENDS.items():
            @pl.when(j == at)
            def _():
                for k, t in pairs:
                    hidden(k, t, t == NF - 1).start()

        for at, ps in FORWARD.items():
            @pl.when(j == at)
            def _():
                for p in ps:
                    late_send(p).start()

        @pl.when(is_mode(1, "s"))
        def _():
            swap(rows, True).start()
            swap(rows, True).wait()

        @pl.when(is_mode(1, "h"))
        def _():
            to_rows(slot_x)
            copy = pltpu.make_async_copy(xv.at[slot_x], sh, s_sem)
            copy.start()
            copy.wait()

        @pl.when(is_mode(1, "v"))
        def _():
            to_rows(0)

        @pl.when(is_mode(1, "r"))
        def _():
            for q in range(M // C):
                @pl.loop(0, C // R)
                def _(r):
                    at = pl.ds(pl.multiple_of(q * C + r * R, R), R)
                    xv[slot_x, at] = acc[at].astype(bf16)
                store(rows - 2, q, slot_x).start()
            for q in range(M // C):
                store(rows - 2, q, slot_x).wait()
                products(rows - 2, q).start()

        @pl.when(j == LEAVE)
        def _():
            @pl.loop(0, M // R)
            def _(r):
                for b in range(acc.shape[1] // FT):
                    buf, k, row = spot(b, gv, uv)
                    at = pl.ds(pl.multiple_of(r * R, R), R)
                    buf[k, pl.ds(pl.multiple_of(row + r * R, R), R)] = acc[at, b * FT:(b + 1) * FT].astype(bf16)
        return step0 + n, word_n, (is_h & (rows < N1)).astype(jnp.int32)

    lax.fori_loop(0, NJ, job, (jnp.int32(0), jnp.int32(words[0]), jnp.int32(0)))

    for q in range(own_rows // C):
        tokens(q).wait_send()
    turn().wait_send()
    for t in range(NF):
        for k in range(3):
            along_y(k, t, width_of(t)).wait_send()
            across(k, t, width_of(t)).wait_send()
    for c in range(ff // WC):
        for k in range(3):
            mine(k, c).wait_send()
    for p in range(len(PIECES)):
        late_send(p).wait_send()
        late_across(p).wait_send()
    for k in range(2):
        for q in range(M // C):
            products(k, q).wait_send()
    for pairs in SENDS.values():
        for k, t in pairs:
            hidden(k, t, t == NF - 1).wait_send()


def write(gv, uv, acc, out, yv, sem):
    step = 128
    early, late = [], []
    for b in range(out.shape[1] // FT):
        buf, k, row = spot(b, gv, uv)
        early.append(pltpu.make_async_copy(buf.at[k, pl.ds(row, M)], out.at[pl.ds(M, M), pl.ds(b * FT, FT)], sem.at[b]))
    for k in range(M // step):
        late.append(pltpu.make_async_copy(yv.at[pl.ds(k * step, step)], out.at[pl.ds(k * step, step)], sem.at[len(early) + k]))
    for copy in early:
        copy.start()
    for k, copy in enumerate(late):
        @pl.loop(0, step // R)
        def _(r):
            at = pl.ds(pl.multiple_of(k * step + r * R, R), R)
            yv[at] = acc[at].astype(jnp.bfloat16)
        copy.start()
    for copy in early + late:
        copy.wait()


def solution(mesh):
    def body(x, wg, wu, wd):
        r, d = x.shape
        kd, ff = wg.shape
        dc = wd.shape[1]
        bf, f32 = jnp.bfloat16, jnp.float32
        any_ = pl.BlockSpec(memory_space=pl.ANY)
        vmem = pl.BlockSpec(memory_space=pltpu.VMEM)
        nh = (2, NF, M, FT)
        shapes = [(2, M, d), (kd, ff), (kd, ff), (ff, dc), (2, kd, ff), (2, kd, ff), (2, ff, dc),
                  (2, ff - L0 * FT, dc), (ff - TURN_ROW, dc), nh, nh, nh]
        dma = pltpu.SemaphoreType.DMA
        nl, nn, nw = len(PIECES), r // C, ff // WC
        work = [jax.ShapeDtypeStruct(s, bf) for s in shapes] + [
            jax.ShapeDtypeStruct((2, M, d), f32), jax.ShapeDtypeStruct((M, d), bf), jax.ShapeDtypeStruct((2, M, d), bf), jax.ShapeDtypeStruct((2, M, d), bf)]
        gv, uv, acc, *_ = pl.pallas_call(
            kernel,
            out_shape=[pltpu.VMEM((2, d, FT), bf)] * 2 + [pltpu.VMEM((M, d), f32)] + work,
            in_specs=[any_] * 4,
            out_specs=[vmem] * 3 + [any_] * len(work),
            scratch_shapes=[
                pltpu.VMEM((2, M, d), bf), pltpu.VMEM((2, FT, d), bf), pltpu.VMEM((2, M, FT), bf),
                dma((3, NF)), dma((3, NF)), dma((3, NF)), dma((3, NF)), dma((3, nw)), dma((3, nw)),
                dma((nl,)), dma((nl,)), dma((nl,)), dma((nl,)), dma((nn,)), dma((nn,)),
                dma((2, M // C)), dma((2, M // C)), dma((2, NF)), dma((2, NF)), dma((2,)),
                dma((2, 7)), dma((2,)), dma, dma((2,)), dma((M // C,)),
            ],
            compiler_params=pltpu.CompilerParams(collective_id=0, has_side_effects=True, vmem_limit_bytes=int(33.9 * 2**20)),
        )(x, wg, wu, wd)
        return pl.pallas_call(
            write,
            out_shape=jax.ShapeDtypeStruct((r, d), bf),
            in_specs=[vmem] * 3,
            out_specs=any_,
            scratch_shapes=[pltpu.VMEM((M, d), bf), dma((28,))],
            compiler_params=pltpu.CompilerParams(vmem_limit_bytes=12 * 2**20),
        )(gv, uv, acc)

    return jax.shard_map(body, mesh=mesh, in_specs=(P(("dp", "tp"), None), P("dp", "tp"), P("dp", "tp"), P("tp", "dp")), out_specs=P(("dp", "tp"), None), check_vma=False)
```

```python
import jax
import jax.numpy as jnp
from jax import lax
from jax.experimental import pallas as pl
from jax.experimental.pallas import tpu as pltpu
from jax.sharding import PartitionSpec as P

MESH = pl.DeviceIdType.MESH
M = 1024
FT = 256
NF = 14
C = 512
WC = 384
NC = 1280
MS = 512
R = 32
L0 = 6
TURN_ROW = 2688
PIECES = ((1536, 512), (2048, 512), (2560, 128), (2688, 128), (2816, 256), (3072, 256), (3328, 128))

O1, O2, N1, N2 = range(4)
MINE, YS, LATE = range(3)
ORDER = (
    "O1M0014Bzs", "O2M0014Bzs", "N1M0014Bz-", "N1Y0005Bk-", "O1Y0005Fk-", "O2Y0005Fk-", "N1Y0501Bkr",
    "N2M0014Bz-", "N2Y0007Bk-", "N1Y0602Fk-", "O1Y0503Fk-", "O2Y0503Fk-", "N2Y0702Bkr", "O1Y0008Sls",
    "O2Y0008Sls", "N1Y0802Fk-", "N2Y0901Fk-", "O1Y0802Fk-", "O2Y0802Fk-", "N1Y1001Fk-", "O1Y1001Fk-",
    "O2Y1001Fk-", "N2Y1001Fk-", "O1Y0803Sl-", "O1L0602Sks", "N1Y1101Fk-", "O1Y1101Fk-", "O2Y1101Fk-",
    "N2Y1101Fk-", "O2Y0804Slh", "N1Y1201Fk-", "N2Y1201Fk-", "O1Y1201Fk-", "O2Y1201Fk-", "O1Y1102Sl-",
    "N2Y1301Fk-", "N1Y1301Fk-", "O1Y1301Fk-", "O2Y1301Fk-", "O1Y1301Sk-", "O1L0802Sk-", "O1L1002Skv",
    "O2Y1202Sh-", "O2L0903Sk-", "O2L1201Sk-", "O2L1301Sk-", "O1-0001Nk-", "O1L1202Sv-",
)
JOBS = tuple((("O1", "O2", "N1", "N2").index(o[:2]), "MYL-".index(o[2]), int(o[3:5]), int(o[5:7]), int(o[7] in "BF"), int(o[7] in "BS"), o[8:])
             for o in ORDER)
NJ = len(JOBS)
AHEAD = {2: (0, 1), 3: (2, 3), 8: (6,)}
FORWARD = {9: (0,), 15: (1,), 19: (2,)}
SENDS = {9: ((0, 6, 2),), 15: ((0, 8, 2),), 16: ((1, 9, 1),), 19: ((0, 10, 1),), 25: ((0, 11, 1),), 28: ((1, 10, 2),),
         31: ((1, 12, 1),), 35: ((1, 13, 1),), 36: ((0, 12, 1), (0, 13, 1))}
TURN = 8
SPREAD = {17: (0,), 35: (1,), 40: (2, 3, 4), 43: (5,), 44: (6,)}
FINAL = (23, 29)
FETCH = 39
LEAVE = 45
SECOND = 12


def plan():
    slots, new, ahead, fresh = [], [], [], []
    group, last, seen, firsts = -1, None, 0, []
    for j, (rows, src, f0, n, s1, s2, _) in enumerate(JOBS):
        starts = bool(s1 and rows != last)
        if starts:
            group, last = group + 1, rows
            firsts.append(j)
        slots.append(max(group, 0) % 2)
        new.append(int(starts))
        top = f0 + n
        fresh.append(max(seen, f0) if src == YS and s1 and top > seen else NF)
        if src == YS and s1:
            seen = max(seen, top)
    late = 2
    load = [-1] * NJ
    for a, b in zip(firsts, firsts[1:]):
        load[b if b == late else a] = JOBS[b][0]
    return slots, new, load, fresh


SLOT, NEW, LOAD, FRESH = plan()
FIELDS = (("rows", 4), ("src", 4), ("f0", 16), ("n", 16), ("first", 2), ("second", 2), ("slot", 2), ("new", 2), ("load", 8),
          ("fresh", 16), ("before", 8), ("after", 8))


def packed(j):
    rows, src, f0, n, first, second, (before, after) = JOBS[j]
    values = (rows, src, f0, n, first, second, SLOT[j], NEW[j], LOAD[j] + 1, FRESH[j], "kzlhv".index(before), "-srhv".index(after))
    word, scale = 0, 1
    for value, (_, size) in zip(values, FIELDS):
        word, scale = word + value * scale, scale * size
    return word


def unpack(word):
    got = {}
    for name, size in FIELDS:
        got[name], word = lax.rem(word, size), lax.div(word, size)
    return got


def spot(b, gv, uv):
    per = gv.shape[1] // M
    return (gv, uv)[b // (2 * per)], b // per % 2, b % per * M


def kernel(x, wg, wu, wd, gv, uv, acc, gn, pg, pu, pd, yg, yu, yd, ld, xd, ho, hs, hr, sv, sh, prod, part,
           xv, dv, hv,
           y_send, y_recv, d_send, d_recv, w_send, w_recv, l_send, l_recv, e_send, e_recv, n_send, n_recv,
           r_send, r_recv, h_send, h_recv, t_sem, w_load, x_load, s_sem, h_sem, o_sem):
    tp, dp = lax.axis_index("tp"), lax.axis_index("dp")
    to_x = {"tp": tp + 1 - 2 * (tp % 2)}
    to_y = {"tp": tp + 2 - 4 * (tp // 2)}
    to_core = {"dp": 1 - dp}
    kd, ff = wg.shape
    dc = wd.shape[1]
    f32, bf16 = jnp.float32, jnp.bfloat16
    last = (NF - 1) * FT

    barrier = pltpu.get_barrier_semaphore()
    for who in (to_x, to_y, to_core):
        pl.semaphore_signal(barrier, inc=1, device_id=who, device_id_type=MESH)
    pl.semaphore_wait(barrier, 3)

    def remote(src, dst, send, recv, who):
        return pltpu.make_async_remote_copy(
            src_ref=src, dst_ref=dst, send_sem=send, recv_sem=recv, device_id=who, device_id_type=MESH)

    def pick(values, j):
        got = jnp.int32(values[0])
        for k, v in enumerate(values):
            if v != values[0]:
                got = jnp.where(j == k, v, got)
        return got

    def once(cond):
        return lambda fn: lax.fori_loop(0, jnp.where(cond, 1, 0), lambda _, c: (fn(), c)[1], 0)

    def col(t):
        return t * FT if isinstance(t, int) else pl.multiple_of(t * FT, FT)

    def tokens(k):
        return remote(x.at[pl.ds(k * M, M)], gn.at[k], n_send.at[k], n_recv.at[k], to_x)

    def mine(k, c):
        at = c * WC if isinstance(c, int) else pl.multiple_of(c * WC, WC)
        ref, peer = ((wg, pg), (wu, pu), (wd, pd))[k]
        ix = (pl.ds(at, WC),) if k == 2 else (slice(None), pl.ds(at, WC))
        return remote(ref.at[ix], peer.at[ix], w_send.at[k, c], w_recv.at[k, c], to_core)

    def y_tile(k, t, width):
        ref, mirror = ((wg, yg), (wu, yu), (wd, yd))[k]
        span = pl.ds(col(t), width)
        return ref.at[(span,) if k == 2 else (slice(None), span)], mirror.at[(0, span) if k == 2 else (0, slice(None), span)], mirror.at[(1, span) if k == 2 else (1, slice(None), span)]

    def along_y(k, t, width=FT):
        src, dst, _ = y_tile(k, t, width)
        return remote(src, dst, y_send.at[k, t], y_recv.at[k, t], to_y)

    def across(k, t, width=FT):
        _, src, dst = y_tile(k, t, width)
        return remote(src, dst, d_send.at[k, t], d_recv.at[k, t], to_core)

    def width_of(t):
        return ff - last if t == NF - 1 else FT

    def late_send(p):
        row, n = PIECES[p]
        dst = ld.at[0, pl.ds(row - L0 * FT, n)]
        if row < TURN_ROW:
            return remote(yd.at[0, pl.ds(row, n)], dst, l_send.at[p], l_recv.at[p], to_x)
        return remote(xd.at[pl.ds(row - TURN_ROW, n)], dst, l_send.at[p], l_recv.at[p], to_y)

    def late_across(p):
        row, n = PIECES[p]
        at = pl.ds(row - L0 * FT, n)
        return remote(ld.at[0, at], ld.at[1, at], e_send.at[p], e_recv.at[p], to_core)

    def turn():
        return remote(wd.at[pl.ds(TURN_ROW, ff - TURN_ROW)], xd, t_sem.at[0], t_sem.at[1], to_x)

    def hidden(k, t, n):
        at = (k, t, slice(None), pl.ds(NF * FT - ff, ff - last)) if t == NF - 1 else (k, pl.ds(t, n))
        return remote(hs.at[at], hr.at[at], h_send.at[k, t], h_recv.at[k, t], to_x)

    def products(k, q):
        rows = pl.ds(q * C, C)
        return remote(prod.at[k, rows], part.at[k, rows], r_send.at[k, q], r_recv.at[k, q], to_x)

    for k in range(2):
        tokens(k).start()
    turn().start()
    for t in range(NF):
        for k in range(3):
            along_y(k, t, width_of(t)).start()
    for c in range(ff // WC):
        for k in range(3):
            mine(k, c).start()

    def tile_at(f):
        return pl.multiple_of(lax.min(f * FT, ff - FT), 128)

    def halves(extent):
        return [pl.ds(pl.multiple_of(core * extent, 128), extent) for core in (dp, 1 - dp)]

    def load_first(slot, f, src):
        at = tile_at(f)
        copies = []
        for k, (pair, dst) in enumerate((((wg, pg) if src == MINE else (yg.at[0], yg.at[1]), gv),
                                         ((wu, pu) if src == MINE else (yu.at[0], yu.at[1]), uv))):
            for m, (ref, rows) in enumerate(zip(pair, halves(kd))):
                copies.append(pltpu.make_async_copy(ref.at[:, pl.ds(at, FT)], dst.at[slot, rows], w_load.at[slot, 2 * k + m]))
        return copies

    def load_second(slot, f, src):
        at = tile_at(f) if src != LATE else pl.multiple_of(tile_at(f) - L0 * FT, 128)
        pair = {MINE: (wd, pd), YS: (yd.at[0], yd.at[1]), LATE: (ld.at[0], ld.at[1])}[src]
        return [pltpu.make_async_copy(ref.at[pl.ds(at, FT)], dv.at[slot, :, cols], w_load.at[slot, 4 + m])
                for m, (ref, cols) in enumerate(zip(pair, halves(dc)))]

    def load_h(slot, rows, f, src, end=False):
        cols = pl.ds(NF * FT - ff, ff - last) if end else slice(None)
        return pltpu.make_async_copy((hr if src == LATE else ho).at[rows, f, :, cols], hv.at[slot, :, cols], w_load.at[slot, 6])

    def load_x(rows, slot):
        own = pltpu.make_async_copy(x.at[pl.ds(pl.multiple_of(lax.min(rows, 1) * M, M), M)], xv.at[slot], x_load.at[slot])
        other = pltpu.make_async_copy(gn.at[lax.max(rows - 2, 0)], xv.at[slot], x_load.at[slot])
        return own, other

    def start_x(rows, slot):
        @pl.when(rows < N1)
        def _():
            load_x(rows, slot)[0].start()

        @pl.when(rows >= N1)
        def _():
            load_x(rows, slot)[1].start()

    def send_across(t, wait_first=True):
        for k in range(3):
            along_y(k, t, width_of(t)).wait_recv()
        for k in range(3):
            across(k, t, width_of(t)).start()

    def prefetch(slot, rows, src, f, first, second, fresh):
        def start(*groups):
            for copies in groups:
                for copy in copies:
                    copy.start()

        @once(src == MINE)
        def _():
            @pl.when((rows == O1) & (f % 3 != 2) & (f < NF - 1))
            def _():
                for k in range(3):
                    mine(k, (2 * f + 2) // 3).wait_recv()
            start(load_first(slot, f, MINE), load_second(slot, f, MINE))

        @once(src == YS)
        def _():
            @once((first == 1) & (f >= fresh))
            def _():
                early = [t for ts in AHEAD.values() for t in ts]
                to_send = f < NF - 1
                for t in early:
                    to_send = to_send & (f != t)

                @pl.when(to_send)
                def _():
                    for k in range(3):
                        along_y(k, f).wait_recv()
                    for k in range(3):
                        across(k, f).start()

                @pl.when(f < NF - 1)
                def _():
                    for k in range(3):
                        across(k, f).wait_recv()

                @pl.when(f == NF - 1)
                def _():
                    send_across(NF - 1)
                    for k in range(3):
                        across(k, NF - 1, width_of(NF - 1)).wait_recv()

            @pl.when(first == 1)
            def _():
                start(load_first(slot, f, YS))

            @pl.when(first == 0)
            def _():
                load_h(slot, rows, f, YS).start()

            @pl.when(second == 1)
            def _():
                start(load_second(slot, f, YS))

        @once(src == LATE)
        def _():
            for k, t, n in (g for groups in SENDS.values() for g in groups):
                @pl.when((rows == k) & (f == t))
                def _():
                    hidden(k, t, n).wait_recv()

            @pl.when(f < NF - 1)
            def _():
                load_h(slot, rows, f, LATE).start()

            @pl.when(f == NF - 1)
            def _():
                hv[slot, :, pl.ds(0, NF * FT - ff)] = jnp.zeros((M, NF * FT - ff), bf16)
                load_h(slot, rows, NF - 1, LATE, True).start()
            for t in range(L0, NF):
                @pl.when((rows == (O1 if t < SECOND else O2)) & (f == t))
                def _():
                    for p, (row, _) in enumerate(PIECES):
                        if row // FT == t:
                            late_across(p).wait_recv()
            start(load_second(slot, f, LATE))

    def store_h(slot, rows, f):
        return (pltpu.make_async_copy(hv.at[slot], ho.at[lax.min(rows, 1), f], h_sem.at[slot]),
                pltpu.make_async_copy(hv.at[slot], hs.at[lax.max(rows - 2, 0), f], h_sem.at[slot]))

    def swap(k, out):
        return pltpu.make_async_copy(acc, sv.at[k], s_sem) if out else pltpu.make_async_copy(sv.at[k], acc, s_sem)

    def store(k, q, slot):
        rows = pl.ds(q * C, C)
        return pltpu.make_async_copy(xv.at[slot, rows], prod.at[k, rows], o_sem.at[q])

    start_x(jnp.int32(O1), 0)
    prefetch(0, jnp.int32(O1), jnp.int32(MINE), jnp.int32(0), jnp.int32(1), jnp.int32(1), jnp.int32(NF))

    words = [packed(j) for j in range(NJ)]

    def job(j, carry):
        step0, word, own_h_before = carry
        this = unpack(word)
        rows, src, f0, n, first, second = (this[k] for k in ("rows", "src", "f0", "n", "first", "second"))
        word_n = pick(words[1:] + words[-1:], j)
        nxt = unpack(word_n)
        fresh, slot_x, load_n = this["fresh"], this["slot"], this["load"] - 1
        is_h = (first == 1) & (second == 0)

        def is_mode(at, what):
            return this["after" if at else "before"] == ("-srhv" if at else "kzlhv").index(what)

        for at, tiles in AHEAD.items():
            @once(j == at)
            def _():
                for t in tiles:
                    send_across(t)
        @once(j == 2)
        def _():
            tokens(0).wait_recv()
        @once(j == 6)
        def _():
            tokens(1).wait_recv()
        @once(j == TURN)
        def _():
            turn().wait_recv()
            for p, (row, _) in enumerate(PIECES):
                if row >= TURN_ROW:
                    late_send(p).start()
        for at, ps in SPREAD.items():
            @once(j == at)
            def _():
                for p in ps:
                    late_send(p).wait_recv()
                for p in ps:
                    late_across(p).start()

        new = this["new"] == 1
        @once(j == 2)
        def _():
            start_x(rows, slot_x)

        @pl.when(new)
        def _():
            load_x(rows, slot_x)[0].wait()

        @pl.when((load_n >= 0) & (j != 2))
        def _():
            start_x(load_n, 1 - slot_x)

        @once(j == 2)
        def _():
            start_x(jnp.int32(JOBS[4][0]), 1 - slot_x)

        @once(is_mode(0, "z"))
        def _():
            @pl.loop(0, M // R)
            def _(r):
                acc[pl.ds(pl.multiple_of(r * R, R), R)] = jnp.zeros((R, acc.shape[1]), f32)

        @once(is_mode(0, "l"))
        def _():
            swap(rows, False).start()
            swap(rows, False).wait()

        def to_rows(slot):
            @pl.loop(0, M // R)
            def _(r):
                at = pl.ds(pl.multiple_of(r * R, R), R)
                xv[slot, at] = acc[at].astype(bf16)

        def from_rows(slot):
            @pl.loop(0, M // R)
            def _(r):
                at = pl.ds(pl.multiple_of(r * R, R), R)
                acc[at] = xv[slot, at].astype(f32)

        @once(j == FETCH)
        def _():
            pltpu.make_async_copy(sh, xv.at[1], x_load.at[1]).start()

        @once(is_mode(0, "h"))
        def _():
            pltpu.make_async_copy(sh, xv.at[1], x_load.at[1]).wait()
            from_rows(1)

        @once(is_mode(0, "v"))
        def _():
            from_rows(0)

        for k, at_job in enumerate(FINAL):
            @once(j == at_job)
            def _():
                for q in range(M // C):
                    products(k, q).wait_recv()
                for ref in (x.at[pl.ds(k * M, M)], part.at[k]):
                    copy = pltpu.make_async_copy(ref, xv.at[slot_x], x_load.at[slot_x])
                    copy.start()
                    copy.wait()

                    @pl.loop(0, M // R)
                    def _(r):
                        at = pl.ds(pl.multiple_of(r * R, R), R)
                        acc[at] = acc[at] + xv[slot_x, at].astype(f32)

        def step(i, _):
            f = f0 + i
            slot = (step0 + i) % 2
            ends = i + 1 == n

            @pl.when(jnp.where(i == 0, own_h_before == 1, is_h))
            def _():
                store_h(1 - slot, rows, f)[0].wait()

            @pl.when(first == 1)
            def _():
                for copy in load_first(slot, f, MINE):
                    copy.wait()

            @pl.when(second == 1)
            def _():
                for copy in load_second(slot, f, MINE):
                    copy.wait()

            half_h = (src == LATE) & (f == NF - 1)

            @pl.when((first == 0) & (second == 1) & jnp.logical_not(half_h))
            def _():
                load_h(slot, rows, f, YS).wait()

            @pl.when(half_h)
            def _():
                load_h(slot, rows, f, YS, True).wait()

            @pl.when(jnp.logical_not(ends & (j == NJ - 1)))
            def _():
                prefetch(1 - slot, *[jnp.where(ends, nxt[k], f + 1 if k == "f0" else this[k])
                                     for k in ("rows", "src", "f0", "first", "second", "fresh")])

            @pl.when(first == 1)
            def _():
                skip = lax.max(f * FT - (ff - FT), 0)
                own = lax.broadcasted_iota(jnp.int32, (MS, FT), 1) >= skip
                for r in range(0, M, MS):
                    at = slice(r, r + MS)
                    a = jnp.dot(xv[slot_x, at], gv[slot], preferred_element_type=f32)
                    b = jnp.dot(xv[slot_x, at], uv[slot], preferred_element_type=f32)
                    hv[slot, at] = jnp.where(own, a * jax.nn.sigmoid(a) * b, 0.0).astype(bf16)

            @pl.when(second == 1)
            def _():
                for c in range(0, acc.shape[1], NC):
                    cols = slice(c, c + NC)
                    acc[:, cols] += jnp.dot(hv[slot], dv[slot, :, cols], preferred_element_type=f32)

            @pl.when(is_h & (rows < N1))
            def _():
                store_h(slot, rows, f)[0].start()

            @pl.when(is_h & (rows >= N1))
            def _():
                store_h(slot, rows, f)[1].start()
            return 0

        lax.fori_loop(0, n, step, 0)

        @pl.when(is_h & (rows >= N1))
        def _():
            store_h((step0 + n - 1) % 2, rows, f0)[1].wait()

        for at, pairs in SENDS.items():
            @once(j == at)
            def _():
                for k, t, n in pairs:
                    hidden(k, t, n).start()

        for at, ps in FORWARD.items():
            @once(j == at)
            def _():
                for p in ps:
                    late_send(p).start()

        @once(is_mode(1, "s"))
        def _():
            swap(rows, True).start()
            swap(rows, True).wait()

        @once(is_mode(1, "h"))
        def _():
            to_rows(slot_x)
            copy = pltpu.make_async_copy(xv.at[slot_x], sh, s_sem)
            copy.start()
            copy.wait()

        @once(is_mode(1, "v"))
        def _():
            to_rows(0)

        @once(is_mode(1, "r"))
        def _():
            for q in range(M // C):
                @pl.loop(0, C // R)
                def _(r):
                    at = pl.ds(pl.multiple_of(q * C + r * R, R), R)
                    xv[slot_x, at] = acc[at].astype(bf16)
                store(rows - 2, q, slot_x).start()
            for q in range(M // C):
                store(rows - 2, q, slot_x).wait()
                products(rows - 2, q).start()

        @once(j == LEAVE)
        def _():
            @pl.loop(0, M // R)
            def _(r):
                for b in range(acc.shape[1] // FT):
                    buf, k, row = spot(b, gv, uv)
                    at = pl.ds(pl.multiple_of(r * R, R), R)
                    buf[k, pl.ds(pl.multiple_of(row + r * R, R), R)] = acc[at, b * FT:(b + 1) * FT].astype(bf16)
        return step0 + n, word_n, (is_h & (rows < N1)).astype(jnp.int32)

    lax.fori_loop(0, NJ, job, (jnp.int32(0), jnp.int32(words[0]), jnp.int32(0)))

    for k in range(2):
        tokens(k).wait_send()
    turn().wait_send()
    for t in range(NF):
        for k in range(3):
            along_y(k, t, width_of(t)).wait_send()
            across(k, t, width_of(t)).wait_send()
    for c in range(ff // WC):
        for k in range(3):
            mine(k, c).wait_send()
    for p in range(len(PIECES)):
        late_send(p).wait_send()
        late_across(p).wait_send()
    for k in range(2):
        for q in range(M // C):
            products(k, q).wait_send()
    for pairs in SENDS.values():
        for k, t, n in pairs:
            hidden(k, t, n).wait_send()


def write(gv, uv, acc, out, yv, sem):
    step = 128
    early, late = [], []
    for b in range(out.shape[1] // FT):
        buf, k, row = spot(b, gv, uv)
        early.append(pltpu.make_async_copy(buf.at[k, pl.ds(row, M)], out.at[pl.ds(M, M), pl.ds(b * FT, FT)], sem.at[b]))
    for k in range(M // step):
        late.append(pltpu.make_async_copy(yv.at[pl.ds(k * step, step)], out.at[pl.ds(k * step, step)], sem.at[len(early) + k]))
    for copy in early:
        copy.start()
    for k, copy in enumerate(late):
        @pl.loop(0, step // R)
        def _(r):
            at = pl.ds(pl.multiple_of(k * step + r * R, R), R)
            yv[at] = acc[at].astype(jnp.bfloat16)
        copy.start()
    for copy in early + late:
        copy.wait()


def solution(mesh):
    def body(x, wg, wu, wd):
        r, d = x.shape
        kd, ff = wg.shape
        dc = wd.shape[1]
        bf, f32 = jnp.bfloat16, jnp.float32
        any_ = pl.BlockSpec(memory_space=pl.ANY)
        vmem = pl.BlockSpec(memory_space=pltpu.VMEM)
        nh = (2, NF, M, FT)
        shapes = [(2, M, d), (kd, ff), (kd, ff), (ff, dc), (2, kd, ff), (2, kd, ff), (2, ff, dc),
                  (2, ff - L0 * FT, dc), (ff - TURN_ROW, dc), nh, nh, nh]
        dma = pltpu.SemaphoreType.DMA
        nl, nn, nw = len(PIECES), r // M, ff // WC
        work = [jax.ShapeDtypeStruct(s, bf) for s in shapes] + [
            jax.ShapeDtypeStruct((2, M, d), f32), jax.ShapeDtypeStruct((M, d), bf), jax.ShapeDtypeStruct((2, M, d), bf), jax.ShapeDtypeStruct((2, M, d), bf)]
        gv, uv, acc, *_ = pl.pallas_call(
            kernel,
            out_shape=[pltpu.VMEM((2, d, FT), bf)] * 2 + [pltpu.VMEM((M, d), f32)] + work,
            in_specs=[any_] * 4,
            out_specs=[vmem] * 3 + [any_] * len(work),
            scratch_shapes=[
                pltpu.VMEM((2, M, d), bf), pltpu.VMEM((2, FT, d), bf), pltpu.VMEM((2, M, FT), bf),
                dma((3, NF)), dma((3, NF)), dma((3, NF)), dma((3, NF)), dma((3, nw)), dma((3, nw)),
                dma((nl,)), dma((nl,)), dma((nl,)), dma((nl,)), dma((nn,)), dma((nn,)),
                dma((2, M // C)), dma((2, M // C)), dma((2, NF)), dma((2, NF)), dma((2,)),
                dma((2, 7)), dma((2,)), dma, dma((2,)), dma((M // C,)),
            ],
            compiler_params=pltpu.CompilerParams(collective_id=0, has_side_effects=True, vmem_limit_bytes=int(33.9 * 2**20)),
        )(x, wg, wu, wd)
        return pl.pallas_call(
            write,
            out_shape=jax.ShapeDtypeStruct((r, d), bf),
            in_specs=[vmem] * 3,
            out_specs=any_,
            scratch_shapes=[pltpu.VMEM((M, d), bf), dma((28,))],
            compiler_params=pltpu.CompilerParams(vmem_limit_bytes=12 * 2**20),
        )(gv, uv, acc)

    return jax.shard_map(body, mesh=mesh, in_specs=(P(("dp", "tp"), None), P("dp", "tp"), P("dp", "tp"), P("tp", "dp")), out_specs=P(("dp", "tp"), None), check_vma=False)
```

```python
import jax
import jax.numpy as jnp
from jax import lax
from jax.experimental import pallas as pl
from jax.experimental.pallas import tpu as pltpu
from jax.sharding import PartitionSpec as P

MESH = pl.DeviceIdType.MESH
M = 1024
FT = 256
NF = 14
C = 256
WC = 384
NC = 1280
MS = 512
R = 32
L0 = 6
TURN_ROW = 2688
PIECES = ((1536, 256), (1792, 256), (2048, 256), (2304, 256), (2560, 128), (2688, 128), (2816, 256), (3072, 256), (3328, 128))

O1, O2, N1, N2 = range(4)
MINE, YS, LATE = range(3)
ORDER = (
    "O1M0014Bzs", "O2M0014Bzs", "N1M0014Bz-", "N1Y0005Bk-", "O1Y0005Fk-", "O2Y0005Fk-", "N1Y0501Bkr",
    "N2M0014Bz-", "N2Y0007Bk-", "N1Y0602Fk-", "N2Y0702Bkr", "O1Y0503Fk-", "O2Y0503Fk-", "O1Y0008Sls",
    "O2Y0008Sls", "N1Y0802Fk-", "N2Y0901Fk-", "O1Y0802Fk-", "O2Y0802Fk-", "N1Y1001Fk-", "O1Y1001Fk-",
    "O2Y1001Fk-", "N2Y1001Fk-", "O1Y0803Sl-", "O1L0602Sks", "N1Y1101Fk-", "O1Y1101Fk-", "O2Y1101Fk-",
    "N2Y1101Fk-", "O2Y0804Slh", "N1Y1201Fk-", "N2Y1201Fk-", "O1Y1201Fk-", "O2Y1201Fk-", "O1Y1102Sl-",
    "N2Y1301Fk-", "N1Y1301Fk-", "O1Y1301Fk-", "O2Y1301Fk-", "O1Y1301Sk-", "O1L0802Sk-", "O1L1002Skv",
    "O2Y1202Sh-", "O2L0903Sk-", "O2L1201Sk-", "O2L1301Sk-", "O1-0001Nk-", "O1L1202Sv-",
)
JOBS = tuple((("O1", "O2", "N1", "N2").index(o[:2]), "MYL-".index(o[2]), int(o[3:5]), int(o[5:7]), int(o[7] in "BF"), int(o[7] in "BS"), o[8:])
             for o in ORDER)
NJ = len(JOBS)
AHEAD = {2: (0, 1), 3: (2, 3), 8: (6,)}
FORWARD = {9: (0, 1), 15: (2, 3), 19: (4,)}
SENDS = {9: ((0, 6), (0, 7)), 15: ((0, 8), (0, 9)), 16: ((1, 9),), 19: ((0, 10),), 25: ((0, 11),), 28: ((1, 10), (1, 11)),
         31: ((1, 12),), 35: ((1, 13),), 36: ((0, 12), (0, 13))}
TURN = 8
SPREAD = {17: (0, 1), 35: (2, 3), 40: (4, 5, 6), 43: (7,), 44: (8,)}
FINAL = (23, 29)
FETCH = 39
LEAVE = 45
SECOND = 12


def plan():
    slots, new, ahead, fresh = [], [], [], []
    group, last, seen, firsts = -1, None, 0, []
    for j, (rows, src, f0, n, s1, s2, _) in enumerate(JOBS):
        starts = bool(s1 and rows != last)
        if starts:
            group, last = group + 1, rows
            firsts.append(j)
        slots.append(max(group, 0) % 2)
        new.append(int(starts))
        top = f0 + n
        fresh.append(max(seen, f0) if src == YS and s1 and top > seen else NF)
        if src == YS and s1:
            seen = max(seen, top)
    late = 2
    load = [-1] * NJ
    for a, b in zip(firsts, firsts[1:]):
        load[b if b == late else a] = JOBS[b][0]
    return slots, new, load, fresh


SLOT, NEW, LOAD, FRESH = plan()
FIELDS = (("rows", 4), ("src", 4), ("f0", 16), ("n", 16), ("first", 2), ("second", 2), ("slot", 2), ("new", 2), ("load", 8),
          ("fresh", 16), ("before", 8), ("after", 8))


def packed(j):
    rows, src, f0, n, first, second, (before, after) = JOBS[j]
    values = (rows, src, f0, n, first, second, SLOT[j], NEW[j], LOAD[j] + 1, FRESH[j], "kzlhv".index(before), "-srhv".index(after))
    word, scale = 0, 1
    for value, (_, size) in zip(values, FIELDS):
        word, scale = word + value * scale, scale * size
    return word


def unpack(word):
    got = {}
    for name, size in FIELDS:
        got[name], word = lax.rem(word, size), lax.div(word, size)
    return got


def spot(b, gv, uv):
    per = gv.shape[1] // M
    return (gv, uv)[b // (2 * per)], b // per % 2, b % per * M


def kernel(x, wg, wu, wd, gv, uv, acc, gn, pg, pu, pd, yg, yu, yd, ld, xd, ho, hs, hr, sv, sh, prod, part,
           xv, dv, hv,
           y_send, y_recv, d_send, d_recv, w_send, w_recv, l_send, l_recv, e_send, e_recv, n_send, n_recv,
           r_send, r_recv, h_send, h_recv, t_sem, w_load, x_load, s_sem, h_sem, o_sem):
    tp, dp = lax.axis_index("tp"), lax.axis_index("dp")
    to_x = {"tp": tp + 1 - 2 * (tp % 2)}
    to_y = {"tp": tp + 2 - 4 * (tp // 2)}
    to_core = {"dp": 1 - dp}
    kd, ff = wg.shape
    dc = wd.shape[1]
    f32, bf16 = jnp.float32, jnp.bfloat16
    last = (NF - 1) * FT
    own_rows = x.shape[0]

    barrier = pltpu.get_barrier_semaphore()
    for who in (to_x, to_y, to_core):
        pl.semaphore_signal(barrier, inc=1, device_id=who, device_id_type=MESH)
    pl.semaphore_wait(barrier, 3)

    def remote(src, dst, send, recv, who):
        return pltpu.make_async_remote_copy(
            src_ref=src, dst_ref=dst, send_sem=send, recv_sem=recv, device_id=who, device_id_type=MESH)

    def pick(values, j):
        got = jnp.int32(values[0])
        for k, v in enumerate(values):
            if v != values[0]:
                got = jnp.where(j == k, v, got)
        return got

    def once(cond):
        return lambda fn: lax.fori_loop(0, jnp.where(cond, 1, 0), lambda _, c: (fn(), c)[1], 0)

    def col(t):
        return t * FT if isinstance(t, int) else pl.multiple_of(t * FT, FT)

    def tokens(q):
        return remote(x.at[pl.ds(q * C, C)], gn.at[q // (M // C), pl.ds(q % (M // C) * C, C)], n_send.at[q], n_recv.at[q], to_x)

    def mine(k, c):
        at = c * WC if isinstance(c, int) else pl.multiple_of(c * WC, WC)
        ref, peer = ((wg, pg), (wu, pu), (wd, pd))[k]
        ix = (pl.ds(at, WC),) if k == 2 else (slice(None), pl.ds(at, WC))
        return remote(ref.at[ix], peer.at[ix], w_send.at[k, c], w_recv.at[k, c], to_core)

    def y_tile(k, t, width):
        ref, mirror = ((wg, yg), (wu, yu), (wd, yd))[k]
        span = pl.ds(col(t), width)
        return ref.at[(span,) if k == 2 else (slice(None), span)], mirror.at[(0, span) if k == 2 else (0, slice(None), span)], mirror.at[(1, span) if k == 2 else (1, slice(None), span)]

    def along_y(k, t, width=FT):
        src, dst, _ = y_tile(k, t, width)
        return remote(src, dst, y_send.at[k, t], y_recv.at[k, t], to_y)

    def across(k, t, width=FT):
        _, src, dst = y_tile(k, t, width)
        return remote(src, dst, d_send.at[k, t], d_recv.at[k, t], to_core)

    def width_of(t):
        return ff - last if t == NF - 1 else FT

    def late_send(p):
        row, n = PIECES[p]
        dst = ld.at[0, pl.ds(row - L0 * FT, n)]
        if row < TURN_ROW:
            return remote(yd.at[0, pl.ds(row, n)], dst, l_send.at[p], l_recv.at[p], to_x)
        return remote(xd.at[pl.ds(row - TURN_ROW, n)], dst, l_send.at[p], l_recv.at[p], to_y)

    def late_across(p):
        row, n = PIECES[p]
        at = pl.ds(row - L0 * FT, n)
        return remote(ld.at[0, at], ld.at[1, at], e_send.at[p], e_recv.at[p], to_core)

    def turn():
        return remote(wd.at[pl.ds(TURN_ROW, ff - TURN_ROW)], xd, t_sem.at[0], t_sem.at[1], to_x)

    def hidden(k, t, end=False):
        at = (k, t, slice(None), pl.ds(NF * FT - ff, ff - last)) if end else (k, t)
        return remote(hs.at[at], hr.at[at], h_send.at[k, t], h_recv.at[k, t], to_x)

    def products(k, q):
        rows = pl.ds(q * C, C)
        return remote(prod.at[k, rows], part.at[k, rows], r_send.at[k, q], r_recv.at[k, q], to_x)

    for q in range(own_rows // C):
        tokens(q).start()
    turn().start()
    for t in range(NF):
        for k in range(3):
            along_y(k, t, width_of(t)).start()
    for c in range(ff // WC):
        for k in range(3):
            mine(k, c).start()

    def tile_at(f):
        return pl.multiple_of(lax.min(f * FT, ff - FT), 128)

    def halves(extent):
        return [pl.ds(pl.multiple_of(core * extent, 128), extent) for core in (dp, 1 - dp)]

    def load_first(slot, f, src):
        at = tile_at(f)
        copies = []
        for k, (pair, dst) in enumerate((((wg, pg) if src == MINE else (yg.at[0], yg.at[1]), gv),
                                         ((wu, pu) if src == MINE else (yu.at[0], yu.at[1]), uv))):
            for m, (ref, rows) in enumerate(zip(pair, halves(kd))):
                copies.append(pltpu.make_async_copy(ref.at[:, pl.ds(at, FT)], dst.at[slot, rows], w_load.at[slot, 2 * k + m]))
        return copies

    def load_second(slot, f, src):
        at = tile_at(f) if src != LATE else pl.multiple_of(tile_at(f) - L0 * FT, 128)
        pair = {MINE: (wd, pd), YS: (yd.at[0], yd.at[1]), LATE: (ld.at[0], ld.at[1])}[src]
        return [pltpu.make_async_copy(ref.at[pl.ds(at, FT)], dv.at[slot, :, cols], w_load.at[slot, 4 + m])
                for m, (ref, cols) in enumerate(zip(pair, halves(dc)))]

    def load_h(slot, rows, f, src, end=False):
        cols = pl.ds(NF * FT - ff, ff - last) if end else slice(None)
        return pltpu.make_async_copy((hr if src == LATE else ho).at[rows, f, :, cols], hv.at[slot, :, cols], w_load.at[slot, 6])

    def load_x(rows, slot):
        own = pltpu.make_async_copy(x.at[pl.ds(pl.multiple_of(lax.min(rows, 1) * M, M), M)], xv.at[slot], x_load.at[slot])
        other = pltpu.make_async_copy(gn.at[lax.max(rows - 2, 0)], xv.at[slot], x_load.at[slot])
        return own, other

    def start_x(rows, slot):
        @pl.when(rows < N1)
        def _():
            load_x(rows, slot)[0].start()

        @pl.when(rows >= N1)
        def _():
            load_x(rows, slot)[1].start()

    def send_across(t, wait_first=True):
        for k in range(3):
            along_y(k, t, width_of(t)).wait_recv()
        for k in range(3):
            across(k, t, width_of(t)).start()

    def prefetch(slot, rows, src, f, first, second, fresh):
        def start(*groups):
            for copies in groups:
                for copy in copies:
                    copy.start()

        @once(src == MINE)
        def _():
            @pl.when((rows == O1) & (f % 3 != 2) & (f < NF - 1))
            def _():
                for k in range(3):
                    mine(k, (2 * f + 2) // 3).wait_recv()
            start(load_first(slot, f, MINE), load_second(slot, f, MINE))

        @once(src == YS)
        def _():
            @once((first == 1) & (f >= fresh))
            def _():
                early = [t for ts in AHEAD.values() for t in ts]
                to_send = f < NF - 1
                for t in early:
                    to_send = to_send & (f != t)

                @pl.when(to_send)
                def _():
                    for k in range(3):
                        along_y(k, f).wait_recv()
                    for k in range(3):
                        across(k, f).start()

                @pl.when(f < NF - 1)
                def _():
                    for k in range(3):
                        across(k, f).wait_recv()

                @pl.when(f == NF - 1)
                def _():
                    send_across(NF - 1)
                    for k in range(3):
                        across(k, NF - 1, width_of(NF - 1)).wait_recv()

            @pl.when(first == 1)
            def _():
                start(load_first(slot, f, YS))

            @pl.when(first == 0)
            def _():
                load_h(slot, rows, f, YS).start()

            @pl.when(second == 1)
            def _():
                start(load_second(slot, f, YS))

        @once(src == LATE)
        def _():
            @pl.when(f < NF - 1)
            def _():
                hidden(rows, f).wait_recv()
                load_h(slot, rows, f, LATE).start()

            @pl.when(f == NF - 1)
            def _():
                hidden(rows, NF - 1, True).wait_recv()
                hv[slot, :, pl.ds(0, NF * FT - ff)] = jnp.zeros((M, NF * FT - ff), bf16)
                load_h(slot, rows, NF - 1, LATE, True).start()
            for t in range(L0, NF):
                @pl.when((rows == (O1 if t < SECOND else O2)) & (f == t))
                def _():
                    for p, (row, _) in enumerate(PIECES):
                        if row // FT == t:
                            late_across(p).wait_recv()
            start(load_second(slot, f, LATE))

    def store_h(slot, rows, f):
        return (pltpu.make_async_copy(hv.at[slot], ho.at[lax.min(rows, 1), f], h_sem.at[slot]),
                pltpu.make_async_copy(hv.at[slot], hs.at[lax.max(rows - 2, 0), f], h_sem.at[slot]))

    def swap(k, out):
        return pltpu.make_async_copy(acc, sv.at[k], s_sem) if out else pltpu.make_async_copy(sv.at[k], acc, s_sem)

    def store(k, q, slot):
        rows = pl.ds(q * C, C)
        return pltpu.make_async_copy(xv.at[slot, rows], prod.at[k, rows], o_sem.at[q])

    start_x(jnp.int32(O1), 0)
    prefetch(0, jnp.int32(O1), jnp.int32(MINE), jnp.int32(0), jnp.int32(1), jnp.int32(1), jnp.int32(NF))

    words = [packed(j) for j in range(NJ)]

    def job(j, carry):
        step0, word, own_h_before = carry
        this = unpack(word)
        rows, src, f0, n, first, second = (this[k] for k in ("rows", "src", "f0", "n", "first", "second"))
        word_n = pick(words[1:] + words[-1:], j)
        nxt = unpack(word_n)
        fresh, slot_x, load_n = this["fresh"], this["slot"], this["load"] - 1
        is_h = (first == 1) & (second == 0)

        def is_mode(at, what):
            return this["after" if at else "before"] == ("-srhv" if at else "kzlhv").index(what)

        for at, tiles in AHEAD.items():
            @once(j == at)
            def _():
                for t in tiles:
                    send_across(t)
        @once(j == 2)
        def _():
            for q in range(M // C):
                tokens(q).wait_recv()
        @once(j == 6)
        def _():
            for q in range(M // C, own_rows // C):
                tokens(q).wait_recv()
        @once(j == TURN)
        def _():
            turn().wait_recv()
            for p, (row, _) in enumerate(PIECES):
                if row >= TURN_ROW:
                    late_send(p).start()
        for at, ps in SPREAD.items():
            @once(j == at)
            def _():
                for p in ps:
                    late_send(p).wait_recv()
                for p in ps:
                    late_across(p).start()

        new = this["new"] == 1
        @once(j == 2)
        def _():
            start_x(rows, slot_x)

        @pl.when(new)
        def _():
            load_x(rows, slot_x)[0].wait()

        @pl.when((load_n >= 0) & (j != 2))
        def _():
            start_x(load_n, 1 - slot_x)

        @once(j == 2)
        def _():
            start_x(jnp.int32(JOBS[4][0]), 1 - slot_x)

        @once(is_mode(0, "z"))
        def _():
            @pl.loop(0, M // R)
            def _(r):
                acc[pl.ds(pl.multiple_of(r * R, R), R)] = jnp.zeros((R, acc.shape[1]), f32)

        @once(is_mode(0, "l"))
        def _():
            swap(rows, False).start()
            swap(rows, False).wait()

        def to_rows(slot):
            @pl.loop(0, M // R)
            def _(r):
                at = pl.ds(pl.multiple_of(r * R, R), R)
                xv[slot, at] = acc[at].astype(bf16)

        def from_rows(slot):
            @pl.loop(0, M // R)
            def _(r):
                at = pl.ds(pl.multiple_of(r * R, R), R)
                acc[at] = xv[slot, at].astype(f32)

        @once(j == FETCH)
        def _():
            pltpu.make_async_copy(sh, xv.at[1], x_load.at[1]).start()

        @once(is_mode(0, "h"))
        def _():
            pltpu.make_async_copy(sh, xv.at[1], x_load.at[1]).wait()
            from_rows(1)

        @once(is_mode(0, "v"))
        def _():
            from_rows(0)

        for k, at_job in enumerate(FINAL):
            @once(j == at_job)
            def _():
                for q in range(M // C):
                    products(k, q).wait_recv()
                for ref in (x.at[pl.ds(k * M, M)], part.at[k]):
                    copy = pltpu.make_async_copy(ref, xv.at[slot_x], x_load.at[slot_x])
                    copy.start()
                    copy.wait()

                    @pl.loop(0, M // R)
                    def _(r):
                        at = pl.ds(pl.multiple_of(r * R, R), R)
                        acc[at] = acc[at] + xv[slot_x, at].astype(f32)

        def step(i, _):
            f = f0 + i
            slot = (step0 + i) % 2
            ends = i + 1 == n

            @pl.when(jnp.where(i == 0, own_h_before == 1, is_h))
            def _():
                store_h(1 - slot, rows, f)[0].wait()

            @pl.when(first == 1)
            def _():
                for copy in load_first(slot, f, MINE):
                    copy.wait()

            @pl.when(second == 1)
            def _():
                for copy in load_second(slot, f, MINE):
                    copy.wait()

            half_h = (src == LATE) & (f == NF - 1)

            @pl.when((first == 0) & (second == 1) & jnp.logical_not(half_h))
            def _():
                load_h(slot, rows, f, YS).wait()

            @pl.when(half_h)
            def _():
                load_h(slot, rows, f, YS, True).wait()

            @pl.when(jnp.logical_not(ends & (j == NJ - 1)))
            def _():
                prefetch(1 - slot, *[jnp.where(ends, nxt[k], f + 1 if k == "f0" else this[k])
                                     for k in ("rows", "src", "f0", "first", "second", "fresh")])

            @pl.when(first == 1)
            def _():
                skip = lax.max(f * FT - (ff - FT), 0)
                own = lax.broadcasted_iota(jnp.int32, (MS, FT), 1) >= skip
                for r in range(0, M, MS):
                    at = slice(r, r + MS)
                    a = jnp.dot(xv[slot_x, at], gv[slot], preferred_element_type=f32)
                    b = jnp.dot(xv[slot_x, at], uv[slot], preferred_element_type=f32)
                    hv[slot, at] = jnp.where(own, a * jax.nn.sigmoid(a) * b, 0.0).astype(bf16)

            @pl.when(second == 1)
            def _():
                for c in range(0, acc.shape[1], NC):
                    cols = slice(c, c + NC)
                    acc[:, cols] += jnp.dot(hv[slot], dv[slot, :, cols], preferred_element_type=f32)

            @pl.when(is_h & (rows < N1))
            def _():
                store_h(slot, rows, f)[0].start()

            @pl.when(is_h & (rows >= N1))
            def _():
                store_h(slot, rows, f)[1].start()
            return 0

        lax.fori_loop(0, n, step, 0)

        @pl.when(is_h & (rows >= N1))
        def _():
            store_h((step0 + n - 1) % 2, rows, f0)[1].wait()

        for at, pairs in SENDS.items():
            @once(j == at)
            def _():
                for k, t in pairs:
                    hidden(k, t, t == NF - 1).start()

        for at, ps in FORWARD.items():
            @once(j == at)
            def _():
                for p in ps:
                    late_send(p).start()

        @once(is_mode(1, "s"))
        def _():
            swap(rows, True).start()
            swap(rows, True).wait()

        @once(is_mode(1, "h"))
        def _():
            to_rows(slot_x)
            copy = pltpu.make_async_copy(xv.at[slot_x], sh, s_sem)
            copy.start()
            copy.wait()

        @once(is_mode(1, "v"))
        def _():
            to_rows(0)

        @once(is_mode(1, "r"))
        def _():
            for q in range(M // C):
                @pl.loop(0, C // R)
                def _(r):
                    at = pl.ds(pl.multiple_of(q * C + r * R, R), R)
                    xv[slot_x, at] = acc[at].astype(bf16)
                store(rows - 2, q, slot_x).start()
            for q in range(M // C):
                store(rows - 2, q, slot_x).wait()
                products(rows - 2, q).start()

        @once(j == LEAVE)
        def _():
            @pl.loop(0, M // R)
            def _(r):
                for b in range(acc.shape[1] // FT):
                    buf, k, row = spot(b, gv, uv)
                    at = pl.ds(pl.multiple_of(r * R, R), R)
                    buf[k, pl.ds(pl.multiple_of(row + r * R, R), R)] = acc[at, b * FT:(b + 1) * FT].astype(bf16)
        return step0 + n, word_n, (is_h & (rows < N1)).astype(jnp.int32)

    lax.fori_loop(0, NJ, job, (jnp.int32(0), jnp.int32(words[0]), jnp.int32(0)))

    for q in range(own_rows // C):
        tokens(q).wait_send()
    turn().wait_send()
    for t in range(NF):
        for k in range(3):
            along_y(k, t, width_of(t)).wait_send()
            across(k, t, width_of(t)).wait_send()
    for c in range(ff // WC):
        for k in range(3):
            mine(k, c).wait_send()
    for p in range(len(PIECES)):
        late_send(p).wait_send()
        late_across(p).wait_send()
    for k in range(2):
        for q in range(M // C):
            products(k, q).wait_send()
    for pairs in SENDS.values():
        for k, t in pairs:
            hidden(k, t, t == NF - 1).wait_send()


def write(gv, uv, acc, out, yv, sem):
    step = 128
    early, late = [], []
    for b in range(out.shape[1] // FT):
        buf, k, row = spot(b, gv, uv)
        early.append(pltpu.make_async_copy(buf.at[k, pl.ds(row, M)], out.at[pl.ds(M, M), pl.ds(b * FT, FT)], sem.at[b]))
    for k in range(M // step):
        late.append(pltpu.make_async_copy(yv.at[pl.ds(k * step, step)], out.at[pl.ds(k * step, step)], sem.at[len(early) + k]))
    for copy in early:
        copy.start()
    for k, copy in enumerate(late):
        @pl.loop(0, step // R)
        def _(r):
            at = pl.ds(pl.multiple_of(k * step + r * R, R), R)
            yv[at] = acc[at].astype(jnp.bfloat16)
        copy.start()
    for copy in early + late:
        copy.wait()


def solution(mesh):
    def body(x, wg, wu, wd):
        r, d = x.shape
        kd, ff = wg.shape
        dc = wd.shape[1]
        bf, f32 = jnp.bfloat16, jnp.float32
        any_ = pl.BlockSpec(memory_space=pl.ANY)
        vmem = pl.BlockSpec(memory_space=pltpu.VMEM)
        nh = (2, NF, M, FT)
        shapes = [(2, M, d), (kd, ff), (kd, ff), (ff, dc), (2, kd, ff), (2, kd, ff), (2, ff, dc),
                  (2, ff - L0 * FT, dc), (ff - TURN_ROW, dc), nh, nh, nh]
        dma = pltpu.SemaphoreType.DMA
        nl, nn, nw = len(PIECES), r // C, ff // WC
        work = [jax.ShapeDtypeStruct(s, bf) for s in shapes] + [
            jax.ShapeDtypeStruct((2, M, d), f32), jax.ShapeDtypeStruct((M, d), bf), jax.ShapeDtypeStruct((2, M, d), bf), jax.ShapeDtypeStruct((2, M, d), bf)]
        gv, uv, acc, *_ = pl.pallas_call(
            kernel,
            out_shape=[pltpu.VMEM((2, d, FT), bf)] * 2 + [pltpu.VMEM((M, d), f32)] + work,
            in_specs=[any_] * 4,
            out_specs=[vmem] * 3 + [any_] * len(work),
            scratch_shapes=[
                pltpu.VMEM((2, M, d), bf), pltpu.VMEM((2, FT, d), bf), pltpu.VMEM((2, M, FT), bf),
                dma((3, NF)), dma((3, NF)), dma((3, NF)), dma((3, NF)), dma((3, nw)), dma((3, nw)),
                dma((nl,)), dma((nl,)), dma((nl,)), dma((nl,)), dma((nn,)), dma((nn,)),
                dma((2, M // C)), dma((2, M // C)), dma((2, NF)), dma((2, NF)), dma((2,)),
                dma((2, 7)), dma((2,)), dma, dma((2,)), dma((M // C,)),
            ],
            compiler_params=pltpu.CompilerParams(collective_id=0, has_side_effects=True, vmem_limit_bytes=int(33.9 * 2**20)),
        )(x, wg, wu, wd)
        return pl.pallas_call(
            write,
            out_shape=jax.ShapeDtypeStruct((r, d), bf),
            in_specs=[vmem] * 3,
            out_specs=any_,
            scratch_shapes=[pltpu.VMEM((M, d), bf), dma((28,))],
            compiler_params=pltpu.CompilerParams(vmem_limit_bytes=12 * 2**20),
        )(gv, uv, acc)

    return jax.shard_map(body, mesh=mesh, in_specs=(P(("dp", "tp"), None), P("dp", "tp"), P("dp", "tp"), P("tp", "dp")), out_specs=P(("dp", "tp"), None), check_vma=False)
```
